32 devices in a mesh: cfg: 2 (over x), ta: 16 (over z, y, core).
Axes of the slice: x: 2, y: 2, z: 4, core: 2. Of those that a mesh axis runs over, the one named last changes fastest.
Arguments:
- fine_source: bfloat16 [32, 128, 2, 2, 24, 128], P('cfg', 'ta'), parts along dimension 0, may hold values from -24 to 24
- projectors: bfloat16 [32, 128, 2304], P(('cfg', 'ta')), parts along dimension 0, may hold values from -0.21875 to 0.21875
- stencil_links: bfloat16 [32, 8, 48, 864], P(('cfg', 'ta')), parts along dimension 0, may hold values from -0.21875 to 0.21875
- quark_mass: float32 [2], P('cfg'), parts along dimension 0, may hold values from 1.5 to 3
Outputs:
- solution: float32 [32, 8, 96, 128], P(('cfg', 'ta')), parts along dimension 0
- residual: float32 [32, 8, 96, 128], P(('cfg', 'ta')), parts along dimension 0
The draws below stay inside these ranges and needn't reach their ends.
There are 2 independent parts, one for each index of `cfg`. The reference program is written for one: setup_inputs(seed, part) draws one part's arguments, and reference() takes and returns one part's arrays. A program takes and returns all parts, laid end to end along the dimension named above; each array names one. Nothing has to cross between parts.
All inputs are finite; a program needn't handle non-finite values.
Results may differ from the reference program's by a relative error of at most 0.012.
The reference program's roundings to bfloat16 on the way count: a program that leaves them out, or rounds other values in their place, can miss the bound.
Values may be sent and summed in bfloat16 or wider, within the bound.
No kernel may reach another device: no remote copies, remote signals or barrier semaphores. Data moves between devices by JAX's collectives and lax.ppermute only.
A program may use at most 128 MiB of HBM per device.

```python
import math
import jax
import jax.numpy as jnp
from jax import lax

NV = 24
LX = 4
LY = 2
LZ = 8
YX = 16
RHS = 128
ITERS = 3
CC = 48
LT = 2
PLANES = 16
XY = 8
COLS = 128
FK = 24


def draw_fine_source(key, part):
    shape_full = (PLANES, COLS, 2, 2, FK, RHS)
    key_base = jax.random.fold_in(key, 11)
    first_key = jax.random.fold_in(key_base, 0)
    third_key = jax.random.fold_in(key_base, 2)
    slices = (jnp.arange(PLANES) // LZ).astype(jnp.float32) / max(LT - 1, 1)
    values = jax.random.truncated_normal(first_key, -4.0, 4.0, shape_full)
    scales = jnp.exp(jax.random.uniform(third_key, (PLANES, COLS, 1, 1, 1, 1), minval=math.log(0.25), maxval=math.log(2.5)))
    time_ramp = jnp.exp(math.log(3.0) * slices - 0.5 * math.log(3.0))
    return (values * scales * time_ramp.reshape(PLANES, 1, 1, 1, 1, 1)).astype(jnp.bfloat16)


def steps_of(rng, extent, cuts, low, high):
    loudness, own = 1.0, jax.random.fold_in(rng, 6)
    for axis_at, parts in cuts:
        heights = jnp.exp(jax.random.uniform(jax.random.fold_in(own, axis_at), (parts,), jnp.float32, low / len(cuts), high / len(cuts)))
        loudness = loudness * jnp.repeat(heights, extent[axis_at] // parts).reshape([-1 if axis == axis_at else 1 for axis in range(len(extent))])
    return loudness


def normal_values(own_key, extent, spread, most, pieces=(), held_as=jnp.bfloat16):
    gain = steps_of(own_key, extent, pieces, -0.22, 0.18) if pieces else 1.0
    array = jax.random.normal(own_key, extent, jnp.float32) * spread * gain
    return jnp.minimum(jnp.maximum(array, -most), most).astype(held_as)


def setup_inputs(seed: int = 0, part: int = 0) -> dict:
    key_of = jax.random.split(jax.random.key(seed), 5)
    part_splits = jax.random.split(jax.random.fold_in(key_of[4], part), 5)
    return {
        "fine_source": draw_fine_source(jax.random.fold_in(jax.random.fold_in(key_of[4], part), 71), part),
        "projectors": normal_values(part_splits[1], (PLANES, COLS, 4 * NV * FK), (2 * YX * FK) ** -0.5, 0.21875, ((0, 16),)),
        "stencil_links": normal_values(part_splits[2], (PLANES, XY, CC, 18 * CC), (18 * CC) ** -0.5, 0.21875, ((0, 16),)),
        "quark_mass": jnp.clip(jax.random.uniform(part_splits[3], (1,), jnp.float32, 1.5, 3.0), 1.5, 3.0),
    }


roll_table = ((0, 0), (3, -1), (3, 1), (2, -1), (2, 1), (1, -1), (1, 1), (0, -1), (0, 1))

def restrict_plane(operands):
    fine_plane, proj_plane = operands
    fine_plane = fine_plane.astype(jnp.float32).reshape(XY, YX, 2, 2, FK, RHS)
    proj_plane = proj_plane.astype(jnp.float32).reshape(XY, YX, 2, NV, 2, FK)
    proj_re = proj_plane[:, :, :, :, 0, :]
    proj_im = proj_plane[:, :, :, :, 1, :]
    fine_re = fine_plane[:, :, 0]
    fine_im = fine_plane[:, :, 1]
    highest = lax.Precision.HIGHEST
    result_re = jnp.einsum('sohvk,sohkr->shvr', proj_re, fine_re, precision=highest) + jnp.einsum('sohvk,sohkr->shvr', proj_im, fine_im, precision=highest)
    result_im = jnp.einsum('sohvk,sohkr->shvr', proj_re, fine_im, precision=highest) - jnp.einsum('sohvk,sohkr->shvr', proj_im, fine_re, precision=highest)
    return jnp.stack([result_re, result_im], axis=1).reshape(XY, 2 * CC, RHS)

def apply_operator(vector, stencil_links, quark_mass):
    highest = lax.Precision.HIGHEST
    rounded = lax.optimization_barrier(vector.astype(jnp.bfloat16)).astype(jnp.float32)
    lattice = rounded.reshape(LT, LZ, LY, LX, 2 * CC, RHS)
    link_view = stencil_links.reshape(PLANES, XY, CC, 9, 2, CC)
    total_re = quark_mass[0] * rounded[:, :, :CC]
    total_im = quark_mass[0] * rounded[:, :, CC:]
    for direction in range(9):
        axis_number, offset = roll_table[direction]
        if direction == 0:
            neighbour = lattice
        else:
            neighbour = jnp.roll(lattice, offset, axis=axis_number)
        neighbour = neighbour.reshape(PLANES, XY, 2 * CC, RHS)
        near_re = neighbour[:, :, :CC]
        near_im = neighbour[:, :, CC:]
        link_re = link_view[:, :, :, direction, 0, :].astype(jnp.float32)
        link_im = link_view[:, :, :, direction, 1, :].astype(jnp.float32)
        total_re = total_re + jnp.einsum('psij,psjr->psir', link_re, near_re, precision=highest) - jnp.einsum('psij,psjr->psir', link_im, near_im, precision=highest)
        total_im = total_im + jnp.einsum('psij,psjr->psir', link_re, near_im, precision=highest) + jnp.einsum('psij,psjr->psir', link_im, near_re, precision=highest)
    return jnp.concatenate([total_re, total_im], axis=2)

def inner_product(left, right):
    left_re = left[:, :, :CC]
    left_im = left[:, :, CC:]
    right_re = right[:, :, :CC]
    right_im = right[:, :, CC:]
    return (lax.optimization_barrier(jnp.sum(left_re * right_re + left_im * right_im, axis=(0, 1, 2))), lax.optimization_barrier(jnp.sum(left_re * right_im - left_im * right_re, axis=(0, 1, 2))))

def scaled(vector, factor_re, factor_im):
    vector_re = vector[..., :CC, :]
    vector_im = vector[..., CC:, :]
    return jnp.concatenate([factor_re * vector_re - factor_im * vector_im, factor_re * vector_im + factor_im * vector_re], axis=-2)

def reference(fine_source, projectors, stencil_links, quark_mass):
    source = lax.map(restrict_plane, (fine_source, projectors))
    solution = jnp.zeros_like(source)
    residual = source
    basis_q = []
    basis_p = []
    for iteration in range(ITERS):
        direction = residual
        mapped = apply_operator(residual, stencil_links, quark_mass)
        coeffs = [inner_product(earlier, mapped) for earlier in basis_q]
        for number in range(iteration):
            mapped = mapped - scaled(basis_q[number], coeffs[number][0], coeffs[number][1])
            direction = direction - scaled(basis_p[number], coeffs[number][0], coeffs[number][1])
        squared = inner_product(mapped, mapped)[0]
        factor = 1.0 / jnp.sqrt(squared + 1e-06)
        unit_q = mapped * factor
        unit_p = direction * factor
        alpha_re, alpha_im = inner_product(unit_q, residual)
        solution = solution + scaled(unit_p, alpha_re, alpha_im)
        residual = residual - scaled(unit_q, alpha_re, alpha_im)
        basis_q.append(unit_q)
        basis_p.append(unit_p)
    return (solution, residual)
```

```python
import math

import jax
import jax.numpy as jnp
from jax import lax
from jax.experimental import pallas as pl
from jax.experimental.pallas import tpu as pltpu
from jax.sharding import PartitionSpec as P

LX = 4
LZ = 8
ITERS = 3
LANES = 128

VMEM = pl.BlockSpec(memory_space=pltpu.VMEM)
SMEM = pl.BlockSpec(memory_space=pltpu.SMEM)


def whole_call(body, out_shape, operands, specs, scratch=(), name=None):
    return pl.pallas_call(
        body,
        out_shape=out_shape,
        in_specs=specs,
        out_specs=jax.tree.map(lambda _: VMEM, out_shape),
        scratch_shapes=list(scratch),
        name=name,
    )(*operands)


def unpack_rows(values, rows_ref, pair_count, fine_count):
    column_count = values.shape[0]
    lane = lax.broadcasted_iota(jnp.int32, (column_count, LANES), 1)
    tiles = [values[:, t * LANES:(t + 1) * LANES] for t in range(values.shape[1] // LANES)]

    def window(start, target):
        tile, offset = divmod(start, LANES)
        shift = (target - offset) % LANES
        piece = pltpu.roll(tiles[tile], shift, 1) if shift else tiles[tile]
        if offset + fine_count > LANES:
            after = pltpu.roll(tiles[tile + 1], shift, 1) if shift else tiles[tile + 1]
            piece = jnp.where(lane < target + LANES - offset, piece, after)
        return piece

    for pair in range(pair_count):
        base = (pair * 2 // pair_count) * fine_count
        start = pair * 2 * fine_count
        first = window(start, base)
        second = window(start + fine_count, base + 2 * fine_count)
        row = jnp.where((lane >= base) & (lane < base + fine_count), first, 0.0)
        inside = (lane >= base + 2 * fine_count) & (lane < base + 3 * fine_count)
        row = jnp.where(inside, second, row)
        rows_ref[pl.ds(pair, column_count, stride=pair_count), :] = row


def restrict_kernel(parity_ref, proj_ref, fine_ref, keep_ref, send_ref, rows_a, rows_b):
    plane_count, column_count, _ = proj_ref.shape
    comp_rows = fine_ref.shape[2]
    half = comp_rows // 2
    rhs_count = fine_ref.shape[3]
    fine_count = half // 2
    pair_count = proj_ref.shape[2] // (2 * fine_count)
    parity = parity_ref[0]

    def restrict_plane(plane, rows_ref):
        values = proj_ref[plane].astype(jnp.float32)
        unpack_rows(values, rows_ref, pair_count, fine_count)
        total = jnp.zeros((pair_count, 2 * rhs_count), jnp.float32)
        for column in range(column_count):
            weights = rows_ref[pl.ds(column * pair_count, pair_count), :]
            weights = weights[:, :comp_rows].astype(jnp.bfloat16)
            block = fine_ref[plane, column]
            real, imag = block[:half], block[half:]
            right = jnp.concatenate(
                [
                    jnp.concatenate([real, imag], axis=1),
                    jnp.concatenate([imag, -real], axis=1),
                ],
                axis=0,
            )
            total = total + jnp.dot(weights, right, preferred_element_type=jnp.float32)
        return total

    def step(chip, carry):
        even = restrict_plane(2 * chip, rows_a)
        odd = restrict_plane(2 * chip + 1, rows_b)
        own = jnp.where(parity == 0, even, odd)
        other = jnp.where(parity == 0, odd, even)
        keep_ref[chip, :pair_count] = own[:, :rhs_count]
        keep_ref[chip, pair_count:] = own[:, rhs_count:]
        send_ref[chip, :pair_count] = other[:, :rhs_count]
        send_ref[chip, pair_count:] = other[:, rhs_count:]
        return carry

    lax.fori_loop(0, plane_count // 2, step, 0)


def paired_restriction(fine_source, projectors, comp_count):
    plane_count, local_columns = fine_source.shape[:2]
    rhs_count = fine_source.shape[-1]
    width = projectors.shape[2]
    moved = lax.all_to_all(
        projectors.reshape(plane_count, local_columns, width), "ta", 0, 0, tiled=True
    )
    fine = fine_source.reshape(plane_count, local_columns, 2 * comp_count, rhs_count)
    parity = (lax.axis_index("ta") % 2).astype(jnp.int32).reshape(1)
    part = jax.ShapeDtypeStruct((plane_count // 2, 2 * comp_count, rhs_count), jnp.float32)
    keep, send = whole_call(
        restrict_kernel,
        (part, part),
        (parity, moved, fine),
        [SMEM, VMEM, VMEM],
        [pltpu.VMEM((local_columns * comp_count, LANES), jnp.float32)] * 2,
        name="restrict",
    )
    swap = [(device, device ^ 1) for device in range(plane_count)]
    summed = keep + lax.ppermute(send, "ta", swap)
    groups = [list(range(core, plane_count, 2)) for core in range(2)]
    return lax.all_to_all(summed, "ta", 0, 0, axis_index_groups=groups, tiled=True)


def real_weights(proj_view):
    proj_re = proj_view[..., 0, :]
    proj_im = proj_view[..., 1, :]
    first_row = jnp.stack([proj_re, proj_im], axis=-4)
    second_row = jnp.stack([-proj_im, proj_re], axis=-4)
    return jnp.stack([first_row, second_row], axis=-5)


def general_restriction(fine_source, projectors, comp_count, site_count, block_count):
    null_count = comp_count // 2
    plane_count, local_columns = fine_source.shape[:2]
    fine_count, rhs_count = fine_source.shape[4:]
    moved_proj = lax.all_to_all(projectors, "ta", split_axis=1, concat_axis=0, tiled=True)
    group_size = math.gcd(block_count, local_columns)
    groups = local_columns // group_size
    weights = real_weights(
        moved_proj.reshape(plane_count, groups, group_size, 2, null_count, 2, fine_count)
    )
    fine_local = fine_source.reshape(plane_count, groups, group_size, 2, 2, fine_count, rhs_count)
    partial_sums = jnp.einsum(
        "pmgdchvk,pmgchkr->pmdhvr", weights, fine_local, preferred_element_type=jnp.float32
    )
    partial_sums = partial_sums.reshape(plane_count, groups, 2 * comp_count, rhs_count)
    collected = lax.all_to_all(partial_sums, "ta", split_axis=0, concat_axis=1, tiled=True)
    return jnp.sum(
        collected.reshape(site_count, block_count // group_size, 2 * comp_count, rhs_count), axis=1
    )


def fold(value):
    return jnp.sum(value.reshape(-1, 8, value.shape[-1]), axis=0)


def cross(left, right, half):
    left_re, left_im = left[:half], left[half:]
    right_re, right_im = right[:half], right[half:]
    return (
        fold(left_re * right_re + left_im * right_im),
        fold(left_re * right_im - left_im * right_re),
    )


def operator_kernel(count, near, mass_ref, links_ref, residual_ref, *refs):
    vectors = refs[:near]
    basis = refs[near:near + count]
    mapped_ref, sums_ref, packed_ref = refs[near + count:]
    site_count, comp_count, _ = links_ref.shape
    rhs_count = residual_ref.shape[2]
    line_count = site_count // LX
    mass = mass_ref[0]
    for number in range(near):
        for site in range(site_count):
            real = vectors[number][site, :comp_count]
            imag = vectors[number][site, comp_count:]
            packed_ref[number, site, :comp_count, :rhs_count] = real
            packed_ref[number, site, :comp_count, rhs_count:] = imag
            packed_ref[number, site, comp_count:, :rhs_count] = -imag
            packed_ref[number, site, comp_count:, rhs_count:] = real
    totals = [jnp.zeros((8, rhs_count), jnp.float32) for _ in range(3 + 4 * count)]
    for site in range(site_count):
        line, column = divmod(site, LX)
        places = [
            (0, line, column),
            (0, line, (column + 1) % LX),
            (0, line, (column - 1) % LX),
            (0, (line + 1) % line_count, column),
            (0, (line - 1) % line_count, column),
            (1, line, column),
            (2, line, column),
            (3, line, column),
            (near - 1, line, column),
        ]
        right = jnp.concatenate([packed_ref[n, y * LX + x] for n, y, x in places], axis=0)
        product = jnp.dot(links_ref[site], right, preferred_element_type=jnp.float32)
        own = vectors[0][site].astype(jnp.float32)
        mapped = (
            jnp.concatenate([product[:, :rhs_count], product[:, rhs_count:]], axis=0) + mass * own
        )
        mapped_ref[site] = mapped
        held = residual_ref[site]
        parts = [fold(mapped * mapped), *cross(mapped, held, comp_count)]
        for earlier in basis:
            unit = earlier[site]
            parts += [*cross(unit, mapped, comp_count), *cross(unit, held, comp_count)]
        totals = [total + part for total, part in zip(totals, parts)]
    sums_ref[...] = jnp.concatenate(
        [jnp.sum(total, axis=0, keepdims=True) for total in totals]
        + [jnp.zeros((sums_ref.shape[0] - len(totals), rhs_count), jnp.float32)],
        axis=0,
    )


def scaled(vector, factor_re, factor_im, half):
    vector_re, vector_im = vector[:half], vector[half:]
    return jnp.concatenate(
        [
            factor_re * vector_re - factor_im * vector_im,
            factor_re * vector_im + factor_im * vector_re,
        ],
        axis=0,
    )


def update_kernel(count, last, sums_ref, mapped_ref, residual_ref, *refs):
    refs = list(refs)
    basis_q = [refs.pop(0) for _ in range(count)]
    basis_p = [refs.pop(0) for _ in range(count)]
    solution_ref = refs.pop(0) if count else None
    if last:
        new_solution, new_residual = refs
    else:
        new_solution, new_residual, rounded_ref, unit_q_ref, unit_p_ref = refs
    site_count = mapped_ref.shape[0]
    half = mapped_ref.shape[1] // 2
    sums = jnp.sum(sums_ref[...], axis=0)
    row = lambda index: sums[index:index + 1]
    squared, proj_re, proj_im = row(0), row(1), row(2)
    coefs = []
    for number in range(count):
        coef_re, coef_im, back_re, back_im = (row(3 + 4 * number + part) for part in range(4))
        coefs.append((coef_re, coef_im))
        squared = squared - (coef_re * coef_re + coef_im * coef_im)
        proj_re = proj_re - (coef_re * back_re + coef_im * back_im)
        proj_im = proj_im - (coef_re * back_im - coef_im * back_re)
    factor = 1.0 / jnp.sqrt(squared + 1e-06)
    alpha_re = proj_re * factor
    alpha_im = proj_im * factor
    for site in range(site_count):
        mapped = mapped_ref[site]
        held = residual_ref[site]
        direction = held
        for number, (coef_re, coef_im) in enumerate(coefs):
            mapped = mapped - scaled(basis_q[number][site], coef_re, coef_im, half)
            direction = direction - scaled(basis_p[number][site], coef_re, coef_im, half)
        unit_q = mapped * factor
        unit_p = direction * factor
        change = scaled(unit_p, alpha_re, alpha_im, half)
        new_solution[site] = change if solution_ref is None else solution_ref[site] + change
        held = held - scaled(unit_q, alpha_re, alpha_im, half)
        new_residual[site] = held
        if not last:
            rounded_ref[site] = held.astype(jnp.bfloat16)
            unit_q_ref[site] = unit_q
            unit_p_ref[site] = unit_p


def gather_sums(sums):
    devices = lax.axis_size("ta")
    if devices > 32:
        return lax.psum(sums, "ta")[None]
    copies = jnp.broadcast_to(sums, (devices,) + sums.shape)
    return lax.all_to_all(copies, "ta", 0, 0, tiled=True)


def shards(fine_source, projectors, stencil_links, quark_mass):
    _, site_count, comp_count, _ = stencil_links.shape
    plane_count, local_columns = fine_source.shape[:2]
    rhs_count = fine_source.shape[5]
    block_count = projectors.shape[1] // site_count
    if local_columns * 2 == block_count and local_columns % 8 == 0:
        source = paired_restriction(fine_source, projectors, comp_count)
    else:
        source = general_restriction(
            fine_source, projectors, comp_count, site_count, block_count
        )
    links = stencil_links[0]
    ring = [
        (plane, plane // LZ * LZ + (plane + 1) % LZ) for plane in range(plane_count)
    ]
    back = [(target, origin) for origin, target in ring]
    later = [(plane, (plane + LZ) % plane_count) for plane in range(plane_count)]
    earlier = [(target, origin) for origin, target in later]

    full = jax.ShapeDtypeStruct(source.shape, jnp.float32)
    low = jax.ShapeDtypeStruct(source.shape, jnp.bfloat16)
    rounded = source.astype(jnp.bfloat16)
    residual = source
    total = None
    basis_q, basis_p = [], []
    for iteration in range(ITERS):
        vectors = [rounded, lax.ppermute(rounded, "ta", back), lax.ppermute(rounded, "ta", ring)]
        vectors.append(lax.ppermute(rounded, "ta", earlier))
        if plane_count > 2 * LZ:
            vectors.append(lax.ppermute(rounded, "ta", later))
        near = len(vectors)
        sum_rows = -(-(3 + 4 * iteration) // 8) * 8
        mapped, sums = whole_call(
            lambda *refs: operator_kernel(iteration, near, *refs),
            (full, jax.ShapeDtypeStruct((sum_rows, rhs_count), jnp.float32)),
            (quark_mass, links, residual, *vectors, *basis_q),
            [SMEM] + [VMEM] * (2 + near + iteration),
            [pltpu.VMEM((near, site_count, 2 * comp_count, 2 * rhs_count), jnp.bfloat16)],
            name=f"operator_{iteration}",
        )
        gathered = gather_sums(sums)
        last = iteration == ITERS - 1
        operands = [gathered, mapped, residual, *basis_q, *basis_p]
        if iteration:
            operands.append(total)
        outs = whole_call(
            lambda *refs: update_kernel(iteration, last, *refs),
            (full, full) if last else (full, full, low, full, full),
            operands,
            [VMEM] * len(operands),
            name=f"update_{iteration}",
        )
        total, residual = outs[:2]
        if not last:
            rounded = outs[2]
            basis_q.append(outs[3])
            basis_p.append(outs[4])
    return total[None], residual[None]


def solution(mesh):
    return jax.shard_map(
        shards,
        mesh=mesh,
        in_specs=(
            P("cfg", "ta", None, None, None, None),
            P(("cfg", "ta"), None, None),
            P(("cfg", "ta"), None, None, None),
            P("cfg"),
        ),
        out_specs=(P(("cfg", "ta"), None, None, None), P(("cfg", "ta"), None, None, None)),
        check_vma=False,
    )
```

```python
import math

import jax
import jax.numpy as jnp
from jax import lax
from jax.experimental import pallas as pl
from jax.experimental.pallas import tpu as pltpu
from jax.sharding import PartitionSpec as P

LX = 4
LZ = 8
ITERS = 3
LANES = 128

VMEM = pl.BlockSpec(memory_space=pltpu.VMEM)
SMEM = pl.BlockSpec(memory_space=pltpu.SMEM)


def whole_call(body, out_shape, operands, specs, scratch=(), name=None):
    return pl.pallas_call(
        body,
        out_shape=out_shape,
        in_specs=specs,
        out_specs=jax.tree.map(lambda _: VMEM, out_shape),
        scratch_shapes=list(scratch),
        compiler_params=pltpu.CompilerParams(vmem_limit_bytes=16 * 1024 * 1024),
        name=name,
    )(*operands)


def unpack_rows(values, rows_ref, pair_count, fine_count):
    column_count = values.shape[0]
    lane = lax.broadcasted_iota(jnp.int32, (column_count, LANES), 1)
    tiles = [values[:, t * LANES:(t + 1) * LANES] for t in range(values.shape[1] // LANES)]

    def window(start, target):
        tile, offset = divmod(start, LANES)
        shift = (target - offset) % LANES
        piece = pltpu.roll(tiles[tile], shift, 1) if shift else tiles[tile]
        if offset + fine_count > LANES:
            after = pltpu.roll(tiles[tile + 1], shift, 1) if shift else tiles[tile + 1]
            piece = jnp.where(lane < target + LANES - offset, piece, after)
        return piece

    for pair in range(pair_count):
        base = (pair * 2 // pair_count) * fine_count
        start = pair * 2 * fine_count
        first = window(start, base)
        second = window(start + fine_count, base + 2 * fine_count)
        row = jnp.where((lane >= base) & (lane < base + fine_count), first, 0.0)
        inside = (lane >= base + 2 * fine_count) & (lane < base + 3 * fine_count)
        row = jnp.where(inside, second, row)
        rows_ref[pl.ds(pair, column_count, stride=pair_count), :] = row


def restrict_kernel(parity_ref, proj_ref, fine_ref, other_ref, source_ref, rows_ref):
    chip_count, column_count, _ = proj_ref.shape
    local_count, comp_rows, rhs_count = fine_ref.shape[1:]
    half = comp_rows // 2
    fine_count = half // 2
    pair_count = proj_ref.shape[2] // (2 * fine_count)
    parity = parity_ref[0]

    def step(chip, carry):
        values = proj_ref[chip].astype(jnp.float32)
        for core in range(column_count // local_count):
            unpack_rows(
                values[core * local_count:(core + 1) * local_count],
                rows_ref.at[core],
                pair_count,
                fine_count,
            )
        total = jnp.zeros((pair_count, 2 * rhs_count), jnp.float32)
        for core, ref, index in ((parity, fine_ref, 2 * chip + parity), (1 - parity, other_ref, chip)):
            for column in range(local_count):
                weights = rows_ref[core, pl.ds(column * pair_count, pair_count), :]
                weights = weights[:, :comp_rows].astype(jnp.bfloat16)
                block = ref[index, column]
                real, imag = block[:half], block[half:]
                right = jnp.concatenate(
                    [
                        jnp.concatenate([real, imag], axis=1),
                        jnp.concatenate([imag, -real], axis=1),
                    ],
                    axis=0,
                )
                total = total + jnp.dot(weights, right, preferred_element_type=jnp.float32)
        source_ref[chip, :pair_count] = total[:, :rhs_count]
        source_ref[chip, pair_count:] = total[:, rhs_count:]
        return carry

    lax.fori_loop(0, chip_count, step, 0)


def paired_restriction(fine_source, projectors, comp_count):
    plane_count, local_columns = fine_source.shape[:2]
    rhs_count = fine_source.shape[-1]
    width = projectors.shape[2]
    chip_count = plane_count // 2
    groups = [list(range(core, plane_count, 2)) for core in range(2)]
    moved = lax.all_to_all(
        projectors.reshape(chip_count, 2 * local_columns, width),
        "ta",
        0,
        0,
        axis_index_groups=groups,
        tiled=True,
    )
    core = lax.axis_index("ta") % 2
    fine = fine_source.reshape(plane_count, local_columns, 2 * comp_count, rhs_count)
    given = lax.dynamic_index_in_dim(
        fine.reshape((chip_count, 2) + fine.shape[1:]), 1 - core, axis=1, keepdims=False
    )
    other = lax.ppermute(given, "ta", [(device, device ^ 1) for device in range(plane_count)])
    summed = whole_call(
        restrict_kernel,
        jax.ShapeDtypeStruct((chip_count, 2 * comp_count, rhs_count), jnp.float32),
        (core.astype(jnp.int32).reshape(1), moved, fine, other),
        [SMEM, VMEM, VMEM, VMEM],
        [pltpu.VMEM((2, local_columns * comp_count, LANES), jnp.float32)],
        name="restrict",
    )
    return lax.all_to_all(summed, "ta", 0, 0, axis_index_groups=groups, tiled=True)


def real_weights(proj_view):
    proj_re = proj_view[..., 0, :]
    proj_im = proj_view[..., 1, :]
    first_row = jnp.stack([proj_re, proj_im], axis=-4)
    second_row = jnp.stack([-proj_im, proj_re], axis=-4)
    return jnp.stack([first_row, second_row], axis=-5)


def general_restriction(fine_source, projectors, comp_count, site_count, block_count):
    null_count = comp_count // 2
    plane_count, local_columns = fine_source.shape[:2]
    fine_count, rhs_count = fine_source.shape[4:]
    moved_proj = lax.all_to_all(projectors, "ta", split_axis=1, concat_axis=0, tiled=True)
    group_size = math.gcd(block_count, local_columns)
    groups = local_columns // group_size
    weights = real_weights(
        moved_proj.reshape(plane_count, groups, group_size, 2, null_count, 2, fine_count)
    )
    fine_local = fine_source.reshape(plane_count, groups, group_size, 2, 2, fine_count, rhs_count)
    partial_sums = jnp.einsum(
        "pmgdchvk,pmgchkr->pmdhvr", weights, fine_local, preferred_element_type=jnp.float32
    )
    partial_sums = partial_sums.reshape(plane_count, groups, 2 * comp_count, rhs_count)
    collected = lax.all_to_all(partial_sums, "ta", split_axis=0, concat_axis=1, tiled=True)
    return jnp.sum(
        collected.reshape(site_count, block_count // group_size, 2 * comp_count, rhs_count), axis=1
    )


def fold(value):
    return jnp.sum(value.reshape(-1, 8, value.shape[-1]), axis=0)


def cross(left, right, half):
    left_re, left_im = left[:half], left[half:]
    right_re, right_im = right[:half], right[half:]
    return (
        fold(left_re * right_re + left_im * right_im),
        fold(left_re * right_im - left_im * right_re),
    )


def operator_kernel(count, near, mass_ref, links_ref, residual_ref, *refs):
    vectors = refs[:near]
    basis = refs[near:near + count]
    mapped_ref, sums_ref, packed_ref = refs[near + count:]
    site_count, comp_count, _ = links_ref.shape
    rhs_count = residual_ref.shape[2]
    line_count = site_count // LX
    mass = mass_ref[0]
    for number in range(near):
        for site in range(site_count):
            real = vectors[number][site, :comp_count]
            imag = vectors[number][site, comp_count:]
            packed_ref[number, site, :comp_count, :rhs_count] = real
            packed_ref[number, site, :comp_count, rhs_count:] = imag
            packed_ref[number, site, comp_count:, :rhs_count] = -imag
            packed_ref[number, site, comp_count:, rhs_count:] = real
    totals = [jnp.zeros((8, rhs_count), jnp.float32) for _ in range(3 + 4 * count)]
    for site in range(site_count):
        line, column = divmod(site, LX)
        places = [
            (0, line, column),
            (0, line, (column + 1) % LX),
            (0, line, (column - 1) % LX),
            (0, (line + 1) % line_count, column),
            (0, (line - 1) % line_count, column),
            (1, line, column),
            (2, line, column),
            (3, line, column),
            (near - 1, line, column),
        ]
        right = jnp.concatenate([packed_ref[n, y * LX + x] for n, y, x in places], axis=0)
        product = jnp.dot(links_ref[site], right, preferred_element_type=jnp.float32)
        own = vectors[0][site].astype(jnp.float32)
        mapped = (
            jnp.concatenate([product[:, :rhs_count], product[:, rhs_count:]], axis=0) + mass * own
        )
        mapped_ref[site] = mapped
        held = residual_ref[site]
        parts = [fold(mapped * mapped), *cross(mapped, held, comp_count)]
        for earlier in basis:
            unit = earlier[site]
            parts += [*cross(unit, mapped, comp_count), *cross(unit, held, comp_count)]
        totals = [total + part for total, part in zip(totals, parts)]
    sums = jnp.concatenate(
        [jnp.sum(total, axis=0, keepdims=True) for total in totals]
        + [jnp.zeros((sums_ref.shape[1] - len(totals), rhs_count), jnp.float32)],
        axis=0,
    )
    for copy in range(sums_ref.shape[0]):
        sums_ref[copy] = sums


def scaled(vector, factor_re, factor_im, half):
    vector_re, vector_im = vector[:half], vector[half:]
    return jnp.concatenate(
        [
            factor_re * vector_re - factor_im * vector_im,
            factor_re * vector_im + factor_im * vector_re,
        ],
        axis=0,
    )


def update_kernel(count, last, sums_ref, mapped_ref, residual_ref, *refs):
    refs = list(refs)
    basis_q = [refs.pop(0) for _ in range(count)]
    basis_p = [refs.pop(0) for _ in range(count)]
    solution_ref = refs.pop(0) if count else None
    if last:
        new_solution, new_residual = refs
    else:
        new_solution, new_residual, rounded_ref, unit_q_ref, unit_p_ref = refs
    site_count = mapped_ref.shape[0]
    half = mapped_ref.shape[1] // 2
    sums = jnp.sum(sums_ref[...], axis=0)
    row = lambda index: sums[index:index + 1]
    squared, proj_re, proj_im = row(0), row(1), row(2)
    coefs = []
    for number in range(count):
        coef_re, coef_im, back_re, back_im = (row(3 + 4 * number + part) for part in range(4))
        coefs.append((coef_re, coef_im))
        squared = squared - (coef_re * coef_re + coef_im * coef_im)
        proj_re = proj_re - (coef_re * back_re + coef_im * back_im)
        proj_im = proj_im - (coef_re * back_im - coef_im * back_re)
    factor = 1.0 / jnp.sqrt(squared + 1e-06)
    alpha_re = proj_re * factor
    alpha_im = proj_im * factor
    for site in range(site_count):
        mapped = mapped_ref[site]
        held = residual_ref[site]
        direction = held
        for number, (coef_re, coef_im) in enumerate(coefs):
            mapped = mapped - scaled(basis_q[number][site], coef_re, coef_im, half)
            direction = direction - scaled(basis_p[number][site], coef_re, coef_im, half)
        unit_q = mapped * factor
        unit_p = direction * factor
        change = scaled(unit_p, alpha_re, alpha_im, half)
        new_solution[site] = change if solution_ref is None else solution_ref[site] + change
        held = held - scaled(unit_q, alpha_re, alpha_im, half)
        new_residual[site] = held
        if not last:
            rounded_ref[site] = held.astype(jnp.bfloat16)
            unit_q_ref[site] = unit_q
            unit_p_ref[site] = unit_p


def gather_sums(sums):
    if sums.shape[0] == 1:
        return lax.psum(sums, "ta")
    return lax.all_to_all(sums, "ta", 0, 0, tiled=True)


def shards(fine_source, projectors, stencil_links, quark_mass):
    _, site_count, comp_count, _ = stencil_links.shape
    plane_count, local_columns = fine_source.shape[:2]
    rhs_count = fine_source.shape[5]
    block_count = projectors.shape[1] // site_count
    if local_columns * 2 == block_count and local_columns % 8 == 0:
        source = paired_restriction(fine_source, projectors, comp_count)
    else:
        source = general_restriction(
            fine_source, projectors, comp_count, site_count, block_count
        )
    links = stencil_links[0]
    ring = [
        (plane, plane // LZ * LZ + (plane + 1) % LZ) for plane in range(plane_count)
    ]
    back = [(target, origin) for origin, target in ring]
    later = [(plane, (plane + LZ) % plane_count) for plane in range(plane_count)]
    earlier = [(target, origin) for origin, target in later]

    copies = plane_count if plane_count <= 32 else 1
    full = jax.ShapeDtypeStruct(source.shape, jnp.float32)
    low = jax.ShapeDtypeStruct(source.shape, jnp.bfloat16)
    rounded = source.astype(jnp.bfloat16)
    residual = source
    total = None
    basis_q, basis_p = [], []
    for iteration in range(ITERS):
        vectors = [rounded, lax.ppermute(rounded, "ta", back), lax.ppermute(rounded, "ta", ring)]
        vectors.append(lax.ppermute(rounded, "ta", earlier))
        if plane_count > 2 * LZ:
            vectors.append(lax.ppermute(rounded, "ta", later))
        near = len(vectors)
        sum_rows = -(-(3 + 4 * iteration) // 8) * 8
        mapped, sums = whole_call(
            lambda *refs: operator_kernel(iteration, near, *refs),
            (full, jax.ShapeDtypeStruct((copies, sum_rows, rhs_count), jnp.float32)),
            (quark_mass, links, residual, *vectors, *basis_q),
            [SMEM] + [VMEM] * (2 + near + iteration),
            [pltpu.VMEM((near, site_count, 2 * comp_count, 2 * rhs_count), jnp.bfloat16)],
            name=f"operator_{iteration}",
        )
        gathered = gather_sums(sums)
        last = iteration == ITERS - 1
        operands = [gathered, mapped, residual, *basis_q, *basis_p]
        if iteration:
            operands.append(total)
        outs = whole_call(
            lambda *refs: update_kernel(iteration, last, *refs),
            (full, full) if last else (full, full, low, full, full),
            operands,
            [VMEM] * len(operands),
            name=f"update_{iteration}",
        )
        total, residual = outs[:2]
        if not last:
            rounded = outs[2]
            basis_q.append(outs[3])
            basis_p.append(outs[4])
    return total[None], residual[None]


def solution(mesh):
    return jax.shard_map(
        shards,
        mesh=mesh,
        in_specs=(
            P("cfg", "ta", None, None, None, None),
            P(("cfg", "ta"), None, None),
            P(("cfg", "ta"), None, None, None),
            P("cfg"),
        ),
        out_specs=(P(("cfg", "ta"), None, None, None), P(("cfg", "ta"), None, None, None)),
        check_vma=False,
    )
```

```python
import math

import jax
import jax.numpy as jnp
from jax import lax
from jax.experimental import pallas as pl
from jax.experimental.pallas import tpu as pltpu
from jax.sharding import PartitionSpec as P

LX = 4
LZ = 8
ITERS = 3
LANES = 128

VMEM = pl.BlockSpec(memory_space=pltpu.VMEM)
SMEM = pl.BlockSpec(memory_space=pltpu.SMEM)


def whole_call(body, out_shape, operands, specs, scratch=(), name=None):
    return pl.pallas_call(
        body,
        out_shape=out_shape,
        in_specs=specs,
        out_specs=jax.tree.map(lambda _: VMEM, out_shape),
        scratch_shapes=list(scratch),
        compiler_params=pltpu.CompilerParams(vmem_limit_bytes=6 * 1024 * 1024),
        name=name,
    )(*operands)


def unpack_rows(values, rows_ref, pair_count, fine_count):
    column_count = values.shape[0]
    lane = lax.broadcasted_iota(jnp.int32, (column_count, LANES), 1)
    tiles = [values[:, t * LANES:(t + 1) * LANES] for t in range(values.shape[1] // LANES)]

    def window(start, target):
        tile, offset = divmod(start, LANES)
        shift = (target - offset) % LANES
        piece = pltpu.roll(tiles[tile], shift, 1) if shift else tiles[tile]
        if offset + fine_count > LANES:
            after = pltpu.roll(tiles[tile + 1], shift, 1) if shift else tiles[tile + 1]
            piece = jnp.where(lane < target + LANES - offset, piece, after)
        return piece

    for pair in range(pair_count):
        base = (pair * 2 // pair_count) * fine_count
        start = pair * 2 * fine_count
        first = window(start, base)
        second = window(start + fine_count, base + 2 * fine_count)
        row = jnp.where((lane >= base) & (lane < base + fine_count), first, 0.0)
        inside = (lane >= base + 2 * fine_count) & (lane < base + 3 * fine_count)
        row = jnp.where(inside, second, row)
        rows_ref[pl.ds(pair, column_count, stride=pair_count), :] = row


def split_kernel(device_ref, proj_ref, *out_refs):
    chip = device_ref[0] // 2
    for step, out_ref in enumerate(out_refs):
        out_ref[...] = proj_ref[chip ^ step]


def restrict_kernel(step, device_ref, proj_ref, fine_ref, other_ref, source_ref, rows_ref):
    column_count = proj_ref.shape[0]
    local_count, comp_rows, rhs_count = fine_ref.shape[1:]
    half = comp_rows // 2
    fine_count = half // 2
    pair_count = proj_ref.shape[1] // (2 * fine_count)
    chip = (device_ref[0] // 2) ^ step
    parity = device_ref[0] % 2
    values = proj_ref[...].astype(jnp.float32)
    for core in range(column_count // local_count):
        unpack_rows(
            values[core * local_count:(core + 1) * local_count],
            rows_ref.at[core],
            pair_count,
            fine_count,
        )
    total = jnp.zeros((pair_count, 2 * rhs_count), jnp.float32)
    for core, ref, index in ((parity, fine_ref, 2 * chip + parity), (1 - parity, other_ref, chip)):
        for column in range(local_count):
            weights = rows_ref[core, pl.ds(column * pair_count, pair_count), :]
            weights = weights[:, :comp_rows].astype(jnp.bfloat16)
            block = ref[index, column]
            real, imag = block[:half], block[half:]
            right = jnp.concatenate(
                [
                    jnp.concatenate([real, imag], axis=1),
                    jnp.concatenate([imag, -real], axis=1),
                ],
                axis=0,
            )
            total = total + jnp.dot(weights, right, preferred_element_type=jnp.float32)
    source_ref[:pair_count] = total[:, :rhs_count]
    source_ref[pair_count:] = total[:, rhs_count:]


def join_kernel(steps, device_ref, *refs):
    parts, (source_ref, rounded_ref) = refs[:-2], refs[-2:]
    chip = device_ref[0] // 2
    for step, part in zip(steps, parts):
        source_ref[chip ^ step] = part[...]
        rounded_ref[chip ^ step] = part[...].astype(jnp.bfloat16)


def paired_restriction(fine_source, projectors, comp_count):
    plane_count, local_columns = fine_source.shape[:2]
    rhs_count = fine_source.shape[-1]
    width = projectors.shape[2]
    chip_count = plane_count // 2
    device = lax.axis_index("ta").astype(jnp.int32)
    place = device.reshape(1)
    low = jnp.bfloat16

    def swap(value, bits):
        return lax.ppermute(value, "ta", [(other, other ^ bits) for other in range(plane_count)])

    given = whole_call(
        split_kernel,
        [jax.ShapeDtypeStruct((2 * local_columns, width), low)] * chip_count,
        (place, projectors.reshape(chip_count, 2 * local_columns, width)),
        [SMEM, VMEM],
        name="split",
    )
    order = sorted(range(1, chip_count), key=lambda step: (-(step // 4), -(step // 2)))
    moved = {0: given[0]}
    for step in order:
        moved[step] = swap(given[step], 2 * step)
    fine = fine_source.reshape(plane_count, local_columns, 2 * comp_count, rhs_count)
    halves = fine.reshape((chip_count, 2) + fine.shape[1:])
    other = swap(lax.dynamic_index_in_dim(halves, 1 - device % 2, axis=1, keepdims=False), 1)
    parts = {}
    for step in order + [0]:
        part = whole_call(
            lambda *refs: restrict_kernel(step, *refs),
            jax.ShapeDtypeStruct((2 * comp_count, rhs_count), jnp.float32),
            (place, moved[step], fine, other),
            [SMEM, VMEM, VMEM, VMEM],
            [pltpu.VMEM((2, local_columns * comp_count, LANES), jnp.float32)],
            name=f"restrict_{step}",
        )
        parts[step] = swap(part, 2 * step) if step else part
    shape = (chip_count, 2 * comp_count, rhs_count)
    steps = order + [0]
    return whole_call(
        lambda *refs: join_kernel(steps, *refs),
        (jax.ShapeDtypeStruct(shape, jnp.float32), jax.ShapeDtypeStruct(shape, low)),
        (place, *(parts[step] for step in steps)),
        [SMEM] + [VMEM] * chip_count,
        name="join",
    )


def real_weights(proj_view):
    proj_re = proj_view[..., 0, :]
    proj_im = proj_view[..., 1, :]
    first_row = jnp.stack([proj_re, proj_im], axis=-4)
    second_row = jnp.stack([-proj_im, proj_re], axis=-4)
    return jnp.stack([first_row, second_row], axis=-5)


def general_restriction(fine_source, projectors, comp_count, site_count, block_count):
    null_count = comp_count // 2
    plane_count, local_columns = fine_source.shape[:2]
    fine_count, rhs_count = fine_source.shape[4:]
    moved_proj = lax.all_to_all(projectors, "ta", split_axis=1, concat_axis=0, tiled=True)
    group_size = math.gcd(block_count, local_columns)
    groups = local_columns // group_size
    weights = real_weights(
        moved_proj.reshape(plane_count, groups, group_size, 2, null_count, 2, fine_count)
    )
    fine_local = fine_source.reshape(plane_count, groups, group_size, 2, 2, fine_count, rhs_count)
    partial_sums = jnp.einsum(
        "pmgdchvk,pmgchkr->pmdhvr", weights, fine_local, preferred_element_type=jnp.float32
    )
    partial_sums = partial_sums.reshape(plane_count, groups, 2 * comp_count, rhs_count)
    collected = lax.all_to_all(partial_sums, "ta", split_axis=0, concat_axis=1, tiled=True)
    return jnp.sum(
        collected.reshape(site_count, block_count // group_size, 2 * comp_count, rhs_count), axis=1
    )


def fold(value):
    return jnp.sum(value.reshape(-1, 8, value.shape[-1]), axis=0)


def cross(left, right, half):
    left_re, left_im = left[:half], left[half:]
    right_re, right_im = right[:half], right[half:]
    return (
        fold(left_re * right_re + left_im * right_im),
        fold(left_re * right_im - left_im * right_re),
    )


def operator_kernel(count, near, mass_ref, links_ref, residual_ref, *refs):
    vectors = refs[:near]
    basis = refs[near:near + count]
    mapped_ref, sums_ref, packed_ref = refs[near + count:]
    site_count, comp_count, _ = links_ref.shape
    rhs_count = residual_ref.shape[2]
    line_count = site_count // LX
    mass = mass_ref[0]
    for number in range(near):
        for site in range(site_count):
            real = vectors[number][site, :comp_count]
            imag = vectors[number][site, comp_count:]
            packed_ref[number, site, :comp_count, :rhs_count] = real
            packed_ref[number, site, :comp_count, rhs_count:] = imag
            packed_ref[number, site, comp_count:, :rhs_count] = -imag
            packed_ref[number, site, comp_count:, rhs_count:] = real
    totals = [jnp.zeros((8, rhs_count), jnp.float32) for _ in range(3 + 2 * count)]
    for site in range(site_count):
        line, column = divmod(site, LX)
        places = [
            (0, line, column),
            (0, line, (column + 1) % LX),
            (0, line, (column - 1) % LX),
            (0, (line + 1) % line_count, column),
            (0, (line - 1) % line_count, column),
            (1, line, column),
            (2, line, column),
            (3, line, column),
            (near - 1, line, column),
        ]
        right = jnp.concatenate([packed_ref[n, y * LX + x] for n, y, x in places], axis=0)
        product = jnp.dot(links_ref[site], right, preferred_element_type=jnp.float32)
        own = vectors[0][site].astype(jnp.float32)
        mapped = (
            jnp.concatenate([product[:, :rhs_count], product[:, rhs_count:]], axis=0) + mass * own
        )
        mapped_ref[site] = mapped
        held = residual_ref[site]
        parts = [fold(mapped * mapped), *cross(mapped, held, comp_count)]
        for earlier in basis:
            parts += cross(earlier[site], mapped, comp_count)
        totals = [total + part for total, part in zip(totals, parts)]
    sums = jnp.concatenate(
        [jnp.sum(total, axis=0, keepdims=True) for total in totals]
        + [jnp.zeros((sums_ref.shape[1] - len(totals), rhs_count), jnp.float32)],
        axis=0,
    )
    for copy in range(sums_ref.shape[0]):
        sums_ref[copy] = sums


def scaled(vector, factor_re, factor_im, half):
    vector_re, vector_im = vector[:half], vector[half:]
    return jnp.concatenate(
        [
            factor_re * vector_re - factor_im * vector_im,
            factor_re * vector_im + factor_im * vector_re,
        ],
        axis=0,
    )


def times(left, right):
    return left[0] * right[0] - left[1] * right[1], left[0] * right[1] + left[1] * right[0]


def conj_times(left, right):
    return left[0] * right[0] + left[1] * right[1], left[0] * right[1] - left[1] * right[0]


def minus(left, right):
    return left[0] - right[0], left[1] - right[1]


def update_kernel(count, last, sums_ref, mapped_ref, residual_ref, *refs):
    refs = list(refs)
    basis_q = [refs.pop(0) for _ in range(count)]
    basis_p = [refs.pop(0) for _ in range(count)]
    solution_ref, known_ref = (refs.pop(0), refs.pop(0)) if count else (None, None)
    if last:
        new_solution, new_residual = refs
    else:
        new_solution, new_residual, rounded_ref, unit_q_ref, unit_p_ref, new_known = refs
    site_count = mapped_ref.shape[0]
    half = mapped_ref.shape[1] // 2
    sums = jnp.sum(sums_ref[...], axis=0)

    def row(ref, index):
        return ref[index:index + 1]

    squared = row(sums, 0)
    held_by_new = (row(sums, 1), row(sums, 2))
    coefs = [(row(sums, 3 + 2 * j), row(sums, 4 + 2 * j)) for j in range(count)]
    with_held = [(row(known_ref, 3 * j), row(known_ref, 3 * j + 1)) for j in range(count)]
    short = [row(known_ref, 3 * j + 2) for j in range(count)]
    pairs, place = {}, 3 * count
    for j in range(count):
        for i in range(j):
            pairs[i, j] = (row(known_ref, place), row(known_ref, place + 1))
            place += 2
    for j, coef in enumerate(coefs):
        size = coef[0] * coef[0] + coef[1] * coef[1]
        squared = squared - size * (1.0 + short[j])
        held_by_new = minus(held_by_new, conj_times(coef, with_held[j]))
        for i in range(j):
            squared = squared + 2.0 * conj_times(coefs[i], times(pairs[i, j], coef))[0]
    norm_square = squared + 1e-06
    factor = 1.0 / jnp.sqrt(norm_square)
    alpha = (held_by_new[0] * factor, held_by_new[1] * factor)
    if not last:
        with_new = []
        for j, coef in enumerate(coefs):
            left = (coef[0] * short[j], coef[1] * short[j])
            for i in range(count):
                if i != j:
                    pair = pairs[j, i] if j < i else (pairs[i, j][0], -pairs[i, j][1])
                    left = minus(left, times(pair, coefs[i]))
            with_new.append((left[0] * factor, left[1] * factor))
        new_short = 1e-06 / norm_square
        rows = []
        for j in range(count):
            rows += minus(with_held[j], times(with_new[j], alpha))
            rows.append(short[j])
        rows += [alpha[0] * new_short, alpha[1] * new_short, new_short]
        for j in range(count):
            for i in range(j):
                rows += pairs[i, j]
        for pair in with_new:
            rows += pair
        for index, value in enumerate(rows):
            new_known[index:index + 1] = value
    for site in range(site_count):
        mapped = mapped_ref[site]
        held = residual_ref[site]
        direction = held
        for number, (coef_re, coef_im) in enumerate(coefs):
            mapped = mapped - scaled(basis_q[number][site], coef_re, coef_im, half)
            direction = direction - scaled(basis_p[number][site], coef_re, coef_im, half)
        unit_q = mapped * factor
        unit_p = direction * factor
        change = scaled(unit_p, *alpha, half)
        new_solution[site] = change if solution_ref is None else solution_ref[site] + change
        held = held - scaled(unit_q, *alpha, half)
        new_residual[site] = held
        if not last:
            rounded_ref[site] = held.astype(jnp.bfloat16)
            unit_q_ref[site] = unit_q
            unit_p_ref[site] = unit_p


def gather_sums(sums):
    if sums.shape[0] == 1:
        return lax.psum(sums, "ta")
    return lax.all_to_all(sums, "ta", 0, 0, tiled=True)


def shards(fine_source, projectors, stencil_links, quark_mass):
    _, site_count, comp_count, _ = stencil_links.shape
    plane_count, local_columns = fine_source.shape[:2]
    rhs_count = fine_source.shape[5]
    block_count = projectors.shape[1] // site_count
    chip_count = plane_count // 2
    paired = local_columns * 2 == block_count and local_columns % 8 == 0
    if paired and chip_count & (chip_count - 1) == 0:
        source, rounded = paired_restriction(fine_source, projectors, comp_count)
    else:
        source = general_restriction(
            fine_source, projectors, comp_count, site_count, block_count
        )
        rounded = source.astype(jnp.bfloat16)
    links = stencil_links[0]
    ring = [
        (plane, plane // LZ * LZ + (plane + 1) % LZ) for plane in range(plane_count)
    ]
    back = [(target, origin) for origin, target in ring]
    later = [(plane, (plane + LZ) % plane_count) for plane in range(plane_count)]
    earlier = [(target, origin) for origin, target in later]

    copies = plane_count if plane_count <= 32 else 1
    full = jax.ShapeDtypeStruct(source.shape, jnp.float32)
    low = jax.ShapeDtypeStruct(source.shape, jnp.bfloat16)
    residual = source
    total = None
    basis_q, basis_p = [], []
    for iteration in range(ITERS):
        vectors = [rounded, lax.ppermute(rounded, "ta", back), lax.ppermute(rounded, "ta", ring)]
        vectors.append(lax.ppermute(rounded, "ta", earlier))
        if plane_count > 2 * LZ:
            vectors.append(lax.ppermute(rounded, "ta", later))
        near = len(vectors)
        sum_rows = -(-(3 + 2 * iteration) // 8) * 8
        mapped, sums = whole_call(
            lambda *refs: operator_kernel(iteration, near, *refs),
            (full, jax.ShapeDtypeStruct((copies, sum_rows, rhs_count), jnp.float32)),
            (quark_mass, links, residual, *vectors, *basis_q),
            [SMEM] + [VMEM] * (2 + near + iteration),
            [pltpu.VMEM((near, site_count, 2 * comp_count, 2 * rhs_count), jnp.bfloat16)],
            name=f"operator_{iteration}",
        )
        gathered = gather_sums(sums)
        last = iteration == ITERS - 1
        operands = [gathered, mapped, residual, *basis_q, *basis_p]
        if iteration:
            operands += [total, known]
        known_rows = -(-(3 * (iteration + 1) + iteration * (iteration + 1)) // 8) * 8
        outs = whole_call(
            lambda *refs: update_kernel(iteration, last, *refs),
            (full, full)
            if last
            else (full, full, low, full, full, jax.ShapeDtypeStruct((known_rows, rhs_count), jnp.float32)),
            operands,
            [VMEM] * len(operands),
            name=f"update_{iteration}",
        )
        total, residual = outs[:2]
        if not last:
            rounded = outs[2]
            basis_q.append(outs[3])
            basis_p.append(outs[4])
            known = outs[5]
    return total[None], residual[None]


def solution(mesh):
    return jax.shard_map(
        shards,
        mesh=mesh,
        in_specs=(
            P("cfg", "ta", None, None, None, None),
            P(("cfg", "ta"), None, None),
            P(("cfg", "ta"), None, None, None),
            P("cfg"),
        ),
        out_specs=(P(("cfg", "ta"), None, None, None), P(("cfg", "ta"), None, None, None)),
        check_vma=False,
    )
```

```python
import math

import jax
import jax.numpy as jnp
from jax import lax
from jax.experimental import pallas as pl
from jax.experimental.pallas import tpu as pltpu
from jax.sharding import PartitionSpec as P


LX = 4
LZ = 8
ITERS = 3
LANES = 128
STEPS = (1, 3, 4, 7, 5, 6, 2)

VMEM = pl.BlockSpec(memory_space=pltpu.VMEM)
SMEM = pl.BlockSpec(memory_space=pltpu.SMEM)


def send(value, pairs):
    return lax.ppermute(value, "ta", pairs)


def whole_call(body, out_shape, operands, specs, scratch=()):
    return pl.pallas_call(
        body,
        out_shape=out_shape,
        in_specs=specs,
        out_specs=jax.tree.map(lambda _: VMEM, out_shape),
        scratch_shapes=list(scratch),
        compiler_params=pltpu.CompilerParams(vmem_limit_bytes=6 * 1024 * 1024),
    )(*operands)


def unpack_rows(values, rows_ref, pair_count, fine_count):
    column_count = values.shape[0]
    lane = lax.broadcasted_iota(jnp.int32, (column_count, LANES), 1)
    tiles = [values[:, t * LANES:(t + 1) * LANES] for t in range(values.shape[1] // LANES)]

    def window(start, target):
        tile, offset = divmod(start, LANES)
        shift = (target - offset) % LANES
        piece = pltpu.roll(tiles[tile], shift, 1) if shift else tiles[tile]
        if offset + fine_count > LANES:
            after = pltpu.roll(tiles[tile + 1], shift, 1) if shift else tiles[tile + 1]
            piece = jnp.where(lane < target + LANES - offset, piece, after)
        return piece

    for pair in range(pair_count):
        base = (pair * 2 // pair_count) * fine_count
        start = pair * 2 * fine_count
        first = window(start, base)
        second = window(start + fine_count, base + 2 * fine_count)
        row = jnp.where((lane >= base) & (lane < base + fine_count), first, 0.0)
        inside = (lane >= base + 2 * fine_count) & (lane < base + 3 * fine_count)
        row = jnp.where(inside, second, row)
        rows_ref[pl.ds(pair, column_count, stride=pair_count), :] = row


def step_order(chip_count):
    steps = list(range(1, chip_count))
    return list(STEPS) if sorted(STEPS) == steps else steps


def split_kernel(device_ref, proj_ref, *out_refs):
    chip = device_ref[0] // 2
    for step, out_ref in enumerate(out_refs):
        out_ref[...] = proj_ref[chip ^ step]


def restrict_kernel(step, device_ref, proj_ref, fine_ref, other_ref, source_ref, rows_ref):
    column_count = proj_ref.shape[0]
    local_count, comp_rows, rhs_count = fine_ref.shape[1:]
    half = comp_rows // 2
    fine_count = half // 2
    pair_count = proj_ref.shape[1] // (2 * fine_count)
    chip = (device_ref[0] // 2) ^ step
    parity = device_ref[0] % 2
    values = proj_ref[...].astype(jnp.float32)
    for core in range(column_count // local_count):
        unpack_rows(
            values[core * local_count:(core + 1) * local_count],
            rows_ref.at[core],
            pair_count,
            fine_count,
        )
    total = jnp.zeros((pair_count, 2 * rhs_count), jnp.float32)
    for core, ref, index in ((parity, fine_ref, 2 * chip + parity), (1 - parity, other_ref, chip)):
        for column in range(local_count):
            weights = rows_ref[core, pl.ds(column * pair_count, pair_count), :]
            weights = weights[:, :comp_rows].astype(jnp.bfloat16)
            block = ref[index, column]
            real, imag = block[:half], block[half:]
            right = jnp.concatenate(
                [
                    jnp.concatenate([real, imag], axis=1),
                    jnp.concatenate([imag, -real], axis=1),
                ],
                axis=0,
            )
            total = total + jnp.dot(weights, right, preferred_element_type=jnp.float32)
    source_ref[:pair_count] = total[:, :rhs_count]
    source_ref[pair_count:] = total[:, rhs_count:]


def join_kernel(steps, device_ref, *refs):
    parts, (source_ref, rounded_ref) = refs[:-2], refs[-2:]
    chip = device_ref[0] // 2
    for step, part in zip(steps, parts):
        source_ref[chip ^ step] = part[...]
        rounded_ref[chip ^ step] = part[...].astype(jnp.bfloat16)


def paired_restriction(fine_source, projectors, comp_count):
    plane_count, local_columns = fine_source.shape[:2]
    rhs_count = fine_source.shape[-1]
    width = projectors.shape[2]
    chip_count = plane_count // 2
    device = lax.axis_index("ta").astype(jnp.int32)
    place = device.reshape(1)
    low = jnp.bfloat16

    def swap(value, bits):
        return send(value, [(other, other ^ bits) for other in range(plane_count)])

    given = whole_call(
        split_kernel,
        [jax.ShapeDtypeStruct((2 * local_columns, width), low)] * chip_count,
        (place, projectors.reshape(chip_count, 2 * local_columns, width)),
        [SMEM, VMEM],
    )
    order = step_order(chip_count)
    moved = {0: given[0]}
    for step in order:
        moved[step] = swap(given[step], 2 * step)
    fine = fine_source.reshape(plane_count, local_columns, 2 * comp_count, rhs_count)
    halves = fine.reshape((chip_count, 2) + fine.shape[1:])
    other = swap(lax.dynamic_index_in_dim(halves, 1 - device % 2, axis=1, keepdims=False), 1)
    steps = order + [0]
    parts = {}
    for step in steps:
        part = whole_call(
            lambda *refs: restrict_kernel(step, *refs),
            jax.ShapeDtypeStruct((2 * comp_count, rhs_count), jnp.float32),
            (place, moved[step], fine, other),
            [SMEM, VMEM, VMEM, VMEM],
            [pltpu.VMEM((2, local_columns * comp_count, LANES), jnp.float32)],
        )
        parts[step] = swap(part, 2 * step) if step else part
    shape = (chip_count, 2 * comp_count, rhs_count)
    return whole_call(
        lambda *refs: join_kernel(steps, *refs),
        (jax.ShapeDtypeStruct(shape, jnp.float32), jax.ShapeDtypeStruct(shape, low)),
        (place, *(parts[step] for step in steps)),
        [SMEM] + [VMEM] * chip_count,
    )


def real_weights(proj_view):
    proj_re = proj_view[..., 0, :]
    proj_im = proj_view[..., 1, :]
    first_row = jnp.stack([proj_re, proj_im], axis=-4)
    second_row = jnp.stack([-proj_im, proj_re], axis=-4)
    return jnp.stack([first_row, second_row], axis=-5)


def general_restriction(fine_source, projectors, comp_count, site_count, block_count):
    null_count = comp_count // 2
    plane_count, local_columns = fine_source.shape[:2]
    fine_count, rhs_count = fine_source.shape[4:]
    moved_proj = lax.all_to_all(projectors, "ta", split_axis=1, concat_axis=0, tiled=True)
    group_size = math.gcd(block_count, local_columns)
    groups = local_columns // group_size
    weights = real_weights(
        moved_proj.reshape(plane_count, groups, group_size, 2, null_count, 2, fine_count)
    )
    fine_local = fine_source.reshape(plane_count, groups, group_size, 2, 2, fine_count, rhs_count)
    partial_sums = jnp.einsum(
        "pmgdchvk,pmgchkr->pmdhvr", weights, fine_local, preferred_element_type=jnp.float32
    )
    partial_sums = partial_sums.reshape(plane_count, groups, 2 * comp_count, rhs_count)
    collected = lax.all_to_all(partial_sums, "ta", split_axis=0, concat_axis=1, tiled=True)
    return jnp.sum(
        collected.reshape(site_count, block_count // group_size, 2 * comp_count, rhs_count), axis=1
    )


def fold(value):
    return jnp.sum(value.reshape(-1, 8, value.shape[-1]), axis=0)


def cross(left, right, half):
    left_re, left_im = left[:half], left[half:]
    right_re, right_im = right[:half], right[half:]
    return (
        fold(left_re * right_re + left_im * right_im),
        fold(left_re * right_im - left_im * right_re),
    )


def operator_kernel(count, mass_ref, links_ref, residual_ref, *refs):
    mapped_ref, sums_ref, packed_ref = refs[-3:]
    near = packed_ref.shape[0]
    nearby = refs[:near]
    basis = refs[near:near + count]
    site_count, comp_count, _ = links_ref.shape
    rhs_count = residual_ref.shape[2]
    line_count = site_count // LX
    mass = mass_ref[0]
    for number, vector in enumerate(nearby):
        for site in range(site_count):
            real = vector[site, :comp_count]
            imag = vector[site, comp_count:]
            packed_ref[number, site, :comp_count, :rhs_count] = real
            packed_ref[number, site, :comp_count, rhs_count:] = imag
            packed_ref[number, site, comp_count:, :rhs_count] = -imag
            packed_ref[number, site, comp_count:, rhs_count:] = real
    totals = [jnp.zeros((8, rhs_count), jnp.float32) for _ in range(3 + 2 * count)]
    for site in range(site_count):
        line, column = divmod(site, LX)
        places = [
            (0, line, column),
            (0, line, (column + 1) % LX),
            (0, line, (column - 1) % LX),
            (0, (line + 1) % line_count, column),
            (0, (line - 1) % line_count, column),
            (1, line, column),
            (2, line, column),
            (3, line, column),
            (near - 1, line, column),
        ]
        right = jnp.concatenate([packed_ref[n, y * LX + x] for n, y, x in places], axis=0)
        product = jnp.dot(links_ref[site], right, preferred_element_type=jnp.float32)
        own = nearby[0][site].astype(jnp.float32)
        mapped = (
            jnp.concatenate([product[:, :rhs_count], product[:, rhs_count:]], axis=0) + mass * own
        )
        mapped_ref[site] = mapped
        held = residual_ref[site]
        parts = [fold(mapped * mapped), *cross(mapped, held, comp_count)]
        for earlier in basis:
            parts += cross(earlier[site], mapped, comp_count)
        totals = [total + part for total, part in zip(totals, parts)]
    sums = jnp.concatenate(
        [jnp.sum(total, axis=0, keepdims=True) for total in totals]
        + [jnp.zeros((sums_ref.shape[-2] - len(totals), rhs_count), jnp.float32)],
        axis=0,
    )
    sums_ref[...] = sums


def scaled(vector, factor_re, factor_im, half):
    vector_re, vector_im = vector[:half], vector[half:]
    return jnp.concatenate(
        [
            factor_re * vector_re - factor_im * vector_im,
            factor_re * vector_im + factor_im * vector_re,
        ],
        axis=0,
    )


def times(left, right):
    return left[0] * right[0] - left[1] * right[1], left[0] * right[1] + left[1] * right[0]


def conj_times(left, right):
    return left[0] * right[0] + left[1] * right[1], left[0] * right[1] - left[1] * right[0]


def minus(left, right):
    return left[0] - right[0], left[1] - right[1]


def update_kernel(count, last, parts, *refs):
    refs = list(refs)
    part_refs = [refs.pop(0) for _ in range(parts)]
    mapped_ref, residual_ref = refs.pop(0), refs.pop(0)
    basis_q = [refs.pop(0) for _ in range(count)]
    basis_p = [refs.pop(0) for _ in range(count)]
    solution_ref, known_ref = (refs.pop(0), refs.pop(0)) if count else (None, None)
    if last:
        new_solution, new_residual = refs
    else:
        new_solution, new_residual, rounded_ref, unit_q_ref, unit_p_ref, new_known = refs
    site_count = mapped_ref.shape[0]
    half = mapped_ref.shape[1] // 2
    sums = add_pairs(part_refs)

    def row(ref, index):
        return ref[index:index + 1]

    squared = row(sums, 0)
    held_by_new = (row(sums, 1), row(sums, 2))
    coefs = [(row(sums, 3 + 2 * j), row(sums, 4 + 2 * j)) for j in range(count)]
    with_held = [(row(known_ref, 3 * j), row(known_ref, 3 * j + 1)) for j in range(count)]
    short = [row(known_ref, 3 * j + 2) for j in range(count)]
    pairs, place = {}, 3 * count
    for j in range(count):
        for i in range(j):
            pairs[i, j] = (row(known_ref, place), row(known_ref, place + 1))
            place += 2
    for j, coef in enumerate(coefs):
        size = coef[0] * coef[0] + coef[1] * coef[1]
        squared = squared - size * (1.0 + short[j])
        held_by_new = minus(held_by_new, conj_times(coef, with_held[j]))
        for i in range(j):
            squared = squared + 2.0 * conj_times(coefs[i], times(pairs[i, j], coef))[0]
    norm_square = squared + 1e-06
    factor = 1.0 / jnp.sqrt(norm_square)
    alpha = (held_by_new[0] * factor, held_by_new[1] * factor)
    if not last:
        with_new = []
        for j, coef in enumerate(coefs):
            left = (coef[0] * short[j], coef[1] * short[j])
            for i in range(count):
                if i != j:
                    pair = pairs[j, i] if j < i else (pairs[i, j][0], -pairs[i, j][1])
                    left = minus(left, times(pair, coefs[i]))
            with_new.append((left[0] * factor, left[1] * factor))
        new_short = 1e-06 / norm_square
        rows = []
        for j in range(count):
            rows += minus(with_held[j], times(with_new[j], alpha))
            rows.append(short[j])
        rows += [alpha[0] * new_short, alpha[1] * new_short, new_short]
        for j in range(count):
            for i in range(j):
                rows += pairs[i, j]
        for pair in with_new:
            rows += pair
        for index, value in enumerate(rows):
            new_known[index:index + 1] = value
    for site in range(site_count):
        mapped = mapped_ref[site]
        held = residual_ref[site]
        direction = held
        for number, (coef_re, coef_im) in enumerate(coefs):
            mapped = mapped - scaled(basis_q[number][site], coef_re, coef_im, half)
            direction = direction - scaled(basis_p[number][site], coef_re, coef_im, half)
        unit_q = mapped * factor
        unit_p = direction * factor
        change = scaled(unit_p, *alpha, half)
        new_solution[site] = change if solution_ref is None else solution_ref[site] + change
        held = held - scaled(unit_q, *alpha, half)
        new_residual[site] = held
        if not last:
            rounded_ref[site] = held.astype(jnp.bfloat16)
            unit_q_ref[site] = unit_q
            unit_p_ref[site] = unit_p


def add_pairs(refs):
    values = [ref[...] for ref in refs]
    while len(values) > 1:
        values = [values[i] + values[i + 1] for i in range(0, len(values), 2)]
    return values[0]


def add_kernel(*refs):
    refs[-1][...] = add_pairs(refs[:-1])


def gather_sums(sums, device_count):
    step = 1
    while step < device_count:
        step *= 4
    if step != device_count or device_count > 16:
        return [lax.psum(sums, "ta")]
    while step > 1:
        step //= 4
        parts = [sums]
        for turn in (1, 2, 3):
            pairs = [(device, device ^ (turn * step)) for device in range(device_count)]
            parts.append(send(sums, pairs))
        if step > 1:
            shape = jax.ShapeDtypeStruct(sums.shape, jnp.float32)
            sums = whole_call(add_kernel, shape, parts, [VMEM] * 4)
    return parts


def shards(fine_source, projectors, stencil_links, quark_mass):
    _, site_count, comp_count, _ = stencil_links.shape
    plane_count, local_columns = fine_source.shape[:2]
    rhs_count = fine_source.shape[5]
    block_count = projectors.shape[1] // site_count
    chip_count = plane_count // 2
    paired = local_columns * 2 == block_count and local_columns % 8 == 0
    if paired and chip_count & (chip_count - 1) == 0:
        source, rounded = paired_restriction(fine_source, projectors, comp_count)
    else:
        source = general_restriction(
            fine_source, projectors, comp_count, site_count, block_count
        )
        rounded = source.astype(jnp.bfloat16)
    links = stencil_links[0]
    ring = [
        (plane, plane // LZ * LZ + (plane + 1) % LZ) for plane in range(plane_count)
    ]
    back = [(target, origin) for origin, target in ring]
    later = [(plane, (plane + LZ) % plane_count) for plane in range(plane_count)]
    earlier = [(target, origin) for origin, target in later]

    def shape(*sizes, dtype=jnp.float32):
        return jax.ShapeDtypeStruct(sizes, dtype)

    width = 2 * comp_count
    full = shape(site_count, width, rhs_count)
    low = shape(site_count, width, rhs_count, dtype=jnp.bfloat16)
    residual = source
    total = None
    basis_q, basis_p = [], []
    for iteration in range(ITERS):
        last = iteration == ITERS - 1
        nearby = [rounded, send(rounded, back), send(rounded, ring)]
        nearby.append(send(rounded, earlier))
        if plane_count > 2 * LZ:
            nearby.append(send(rounded, later))
        operands = [quark_mass, links, residual, *nearby, *basis_q]
        mapped, sums = whole_call(
            lambda *refs: operator_kernel(iteration, *refs),
            (full, shape(-(-(3 + 2 * iteration) // 8) * 8, rhs_count)),
            operands,
            [SMEM] + [VMEM] * (len(operands) - 1),
            [pltpu.VMEM((len(nearby), site_count, width, 2 * rhs_count), jnp.bfloat16)],
        )
        parts = gather_sums(sums, plane_count)
        operands = [*parts, mapped, residual, *basis_q, *basis_p]
        if iteration:
            operands += [total, known]
        known_rows = -(-(3 * (iteration + 1) + iteration * (iteration + 1)) // 8) * 8
        results = (full, full)
        if not last:
            results += (low, full, full, shape(known_rows, rhs_count))
        outs = whole_call(
            lambda *refs: update_kernel(iteration, last, len(parts), *refs),
            results,
            operands,
            [VMEM] * len(operands),
        )
        total, residual = outs[:2]
        if not last:
            rounded, known = outs[2], outs[5]
            basis_q.append(outs[3])
            basis_p.append(outs[4])
    return total[None], residual[None]


def solution(mesh):
    return jax.shard_map(
        shards,
        mesh=mesh,
        in_specs=(
            P("cfg", "ta", None, None, None, None),
            P(("cfg", "ta"), None, None),
            P(("cfg", "ta"), None, None, None),
            P("cfg"),
        ),
        out_specs=(P(("cfg", "ta"), None, None, None), P(("cfg", "ta"), None, None, None)),
        check_vma=False,
    )
```

```python
import math

import jax
import jax.numpy as jnp
from jax import lax
from jax.experimental import pallas as pl
from jax.experimental.pallas import tpu as pltpu
from jax.sharding import PartitionSpec as P


LX = 4
LZ = 8
ITERS = 3
LANES = 128
PROJ_STEPS = (6, 3, 7, 1, 5, 2, 4)
SOURCE_STEPS = (6, 3, 7, 5, 4, 1, 2)

VMEM = pl.BlockSpec(memory_space=pltpu.VMEM)
SMEM = pl.BlockSpec(memory_space=pltpu.SMEM)


def send(value, pairs):
    return lax.ppermute(value, "ta", pairs)


def whole_call(body, out_shape, operands, specs, scratch=()):
    return pl.pallas_call(
        body,
        out_shape=out_shape,
        in_specs=specs,
        out_specs=jax.tree.map(lambda _: VMEM, out_shape),
        scratch_shapes=list(scratch),
        compiler_params=pltpu.CompilerParams(vmem_limit_bytes=6 * 1024 * 1024),
    )(*operands)


def unpack_rows(values, rows_ref, pair_count, fine_count):
    column_count = values.shape[0]
    lane = lax.broadcasted_iota(jnp.int32, (column_count, LANES), 1)
    tiles = [values[:, t * LANES:(t + 1) * LANES] for t in range(values.shape[1] // LANES)]

    def window(start, target):
        tile, offset = divmod(start, LANES)
        shift = (target - offset) % LANES
        piece = pltpu.roll(tiles[tile], shift, 1) if shift else tiles[tile]
        if offset + fine_count > LANES:
            after = pltpu.roll(tiles[tile + 1], shift, 1) if shift else tiles[tile + 1]
            piece = jnp.where(lane < target + LANES - offset, piece, after)
        return piece

    for pair in range(pair_count):
        base = (pair * 2 // pair_count) * fine_count
        start = pair * 2 * fine_count
        first = window(start, base)
        second = window(start + fine_count, base + 2 * fine_count)
        row = jnp.where((lane >= base) & (lane < base + fine_count), first, 0.0)
        inside = (lane >= base + 2 * fine_count) & (lane < base + 3 * fine_count)
        row = jnp.where(inside, second, row)
        rows_ref[pl.ds(pair, column_count, stride=pair_count), :] = row


def step_order(chip_count, wanted):
    steps = list(range(1, chip_count))
    return list(wanted) if sorted(wanted) == steps else steps


def split_kernel(device_ref, proj_ref, *out_refs):
    chip = device_ref[0] // 2
    for step, out_ref in enumerate(out_refs):
        out_ref[...] = proj_ref[chip ^ step]


def restrict_kernel(step, device_ref, proj_ref, fine_ref, other_ref, source_ref, rows_ref):
    column_count = proj_ref.shape[0]
    local_count, comp_rows, rhs_count = fine_ref.shape[1:]
    half = comp_rows // 2
    fine_count = half // 2
    pair_count = proj_ref.shape[1] // (2 * fine_count)
    chip = (device_ref[0] // 2) ^ step
    parity = device_ref[0] % 2
    values = proj_ref[...].astype(jnp.float32)
    for core in range(column_count // local_count):
        unpack_rows(
            values[core * local_count:(core + 1) * local_count],
            rows_ref.at[core],
            pair_count,
            fine_count,
        )
    total = jnp.zeros((pair_count, 2 * rhs_count), jnp.float32)
    for core, ref, index in ((parity, fine_ref, 2 * chip + parity), (1 - parity, other_ref, chip)):
        for column in range(local_count):
            weights = rows_ref[core, pl.ds(column * pair_count, pair_count), :]
            weights = weights[:, :comp_rows].astype(jnp.bfloat16)
            block = ref[index, column]
            real, imag = block[:half], block[half:]
            right = jnp.concatenate(
                [
                    jnp.concatenate([real, imag], axis=1),
                    jnp.concatenate([imag, -real], axis=1),
                ],
                axis=0,
            )
            total = total + jnp.dot(weights, right, preferred_element_type=jnp.float32)
    source_ref[:pair_count] = total[:, :rhs_count]
    source_ref[pair_count:] = total[:, rhs_count:]


def join_kernel(steps, device_ref, *refs):
    parts, (source_ref, rounded_ref) = refs[:-2], refs[-2:]
    chip = device_ref[0] // 2
    for step, part in zip(steps, parts):
        source_ref[chip ^ step] = part[...]
        rounded_ref[chip ^ step] = part[...].astype(jnp.bfloat16)


def paired_restriction(fine_source, projectors, comp_count):
    plane_count, local_columns = fine_source.shape[:2]
    rhs_count = fine_source.shape[-1]
    width = projectors.shape[2]
    chip_count = plane_count // 2
    device = lax.axis_index("ta").astype(jnp.int32)
    place = device.reshape(1)
    low = jnp.bfloat16

    def swap(value, bits):
        return send(value, [(other, other ^ bits) for other in range(plane_count)])

    given = whole_call(
        split_kernel,
        [jax.ShapeDtypeStruct((2 * local_columns, width), low)] * chip_count,
        (place, projectors.reshape(chip_count, 2 * local_columns, width)),
        [SMEM, VMEM],
    )
    order = step_order(chip_count, PROJ_STEPS)
    moved = {0: given[0]}
    for step in order:
        moved[step] = swap(given[step], 2 * step)
    fine = fine_source.reshape(plane_count, local_columns, 2 * comp_count, rhs_count)
    halves = fine.reshape((chip_count, 2) + fine.shape[1:])
    other = swap(lax.dynamic_index_in_dim(halves, 1 - device % 2, axis=1, keepdims=False), 1)
    steps = step_order(chip_count, SOURCE_STEPS) + [0]
    parts = {}
    for step in steps:
        part = whole_call(
            lambda *refs: restrict_kernel(step, *refs),
            jax.ShapeDtypeStruct((2 * comp_count, rhs_count), jnp.float32),
            (place, moved[step], fine, other),
            [SMEM, VMEM, VMEM, VMEM],
            [pltpu.VMEM((2, local_columns * comp_count, LANES), jnp.float32)],
        )
        parts[step] = swap(part, 2 * step) if step else part
    shape = (chip_count, 2 * comp_count, rhs_count)
    return whole_call(
        lambda *refs: join_kernel(steps, *refs),
        (jax.ShapeDtypeStruct(shape, jnp.float32), jax.ShapeDtypeStruct(shape, low)),
        (place, *(parts[step] for step in steps)),
        [SMEM] + [VMEM] * chip_count,
    )


def real_weights(proj_view):
    proj_re = proj_view[..., 0, :]
    proj_im = proj_view[..., 1, :]
    first_row = jnp.stack([proj_re, proj_im], axis=-4)
    second_row = jnp.stack([-proj_im, proj_re], axis=-4)
    return jnp.stack([first_row, second_row], axis=-5)


def general_restriction(fine_source, projectors, comp_count, site_count, block_count):
    null_count = comp_count // 2
    plane_count, local_columns = fine_source.shape[:2]
    fine_count, rhs_count = fine_source.shape[4:]
    moved_proj = lax.all_to_all(projectors, "ta", split_axis=1, concat_axis=0, tiled=True)
    group_size = math.gcd(block_count, local_columns)
    groups = local_columns // group_size
    weights = real_weights(
        moved_proj.reshape(plane_count, groups, group_size, 2, null_count, 2, fine_count)
    )
    fine_local = fine_source.reshape(plane_count, groups, group_size, 2, 2, fine_count, rhs_count)
    partial_sums = jnp.einsum(
        "pmgdchvk,pmgchkr->pmdhvr", weights, fine_local, preferred_element_type=jnp.float32
    )
    partial_sums = partial_sums.reshape(plane_count, groups, 2 * comp_count, rhs_count)
    collected = lax.all_to_all(partial_sums, "ta", split_axis=0, concat_axis=1, tiled=True)
    return jnp.sum(
        collected.reshape(site_count, block_count // group_size, 2 * comp_count, rhs_count), axis=1
    )


def fold(value):
    return jnp.sum(value.reshape(-1, 8, value.shape[-1]), axis=0)


def cross(left, right, half):
    left_re, left_im = left[:half], left[half:]
    right_re, right_im = right[:half], right[half:]
    return (
        fold(left_re * right_re + left_im * right_im),
        fold(left_re * right_im - left_im * right_re),
    )


def pack_vector(vector, packed_ref, number):
    half = vector.shape[1] // 2
    rhs_count = vector.shape[2]
    for site in range(vector.shape[0]):
        real = vector[site, :half]
        imag = vector[site, half:]
        packed_ref[number, site, :half, :rhs_count] = real
        packed_ref[number, site, :half, rhs_count:] = imag
        packed_ref[number, site, half:, :rhs_count] = -imag
        packed_ref[number, site, half:, rhs_count:] = real


def stacked(product):
    rhs_count = product.shape[1] // 2
    return jnp.concatenate([product[:, :rhs_count], product[:, rhs_count:]], axis=0)


def slice_kernel(mass_ref, links_ref, own_ref, mapped_ref, packed_ref):
    site_count, _, _ = links_ref.shape
    line_count = site_count // LX
    mass = mass_ref[0]
    pack_vector(own_ref, packed_ref, 0)
    for site in range(site_count):
        line, column = divmod(site, LX)
        places = [
            (line, column),
            (line, (column + 1) % LX),
            (line, (column - 1) % LX),
            ((line + 1) % line_count, column),
            ((line - 1) % line_count, column),
        ]
        right = jnp.concatenate([packed_ref[0, y * LX + x] for y, x in places], axis=0)
        product = jnp.dot(
            links_ref[site, :, :right.shape[0]], right, preferred_element_type=jnp.float32
        )
        mapped_ref[site] = stacked(product) + mass * own_ref[site].astype(jnp.float32)


def remote_kernel(count, near, links_ref, partial_ref, residual_ref, *refs):
    mapped_ref, sums_ref, packed_ref = refs[-3:]
    basis = refs[near:near + count]
    site_count, comp_count, width = links_ref.shape
    rhs_count = residual_ref.shape[2]
    for number in range(near):
        pack_vector(refs[number], packed_ref, number)
    start = width - 8 * comp_count
    spare = start % LANES
    totals = [jnp.zeros((8, rhs_count), jnp.float32) for _ in range(3 + 2 * count)]
    for site in range(site_count):
        blocks = [packed_ref[n, site] for n in (0, 1, 2, near - 1)]
        if spare:
            blocks.insert(0, jnp.zeros((spare, 2 * rhs_count), jnp.bfloat16))
        right = jnp.concatenate(blocks, axis=0)
        product = jnp.dot(
            links_ref[site, :, start - spare:], right, preferred_element_type=jnp.float32
        )
        mapped = partial_ref[site] + stacked(product)
        mapped_ref[site] = mapped
        held = residual_ref[site]
        parts = [fold(mapped * mapped), *cross(mapped, held, comp_count)]
        for earlier in basis:
            parts += cross(earlier[site], mapped, comp_count)
        totals = [total + part for total, part in zip(totals, parts)]
    sums_ref[...] = jnp.concatenate(
        [jnp.sum(total, axis=0, keepdims=True) for total in totals]
        + [jnp.zeros((sums_ref.shape[0] - len(totals), rhs_count), jnp.float32)],
        axis=0,
    )


def scaled(vector, factor_re, factor_im, half):
    vector_re, vector_im = vector[:half], vector[half:]
    return jnp.concatenate(
        [
            factor_re * vector_re - factor_im * vector_im,
            factor_re * vector_im + factor_im * vector_re,
        ],
        axis=0,
    )


def times(left, right):
    return left[0] * right[0] - left[1] * right[1], left[0] * right[1] + left[1] * right[0]


def conj_times(left, right):
    return left[0] * right[0] + left[1] * right[1], left[0] * right[1] - left[1] * right[0]


def minus(left, right):
    return left[0] - right[0], left[1] - right[1]


def update_kernel(count, last, parts, *refs):
    refs = list(refs)
    part_refs = [refs.pop(0) for _ in range(parts)]
    mapped_ref, residual_ref = refs.pop(0), refs.pop(0)
    basis_q = [refs.pop(0) for _ in range(count)]
    basis_p = [refs.pop(0) for _ in range(count)]
    solution_ref, known_ref = (refs.pop(0), refs.pop(0)) if count else (None, None)
    if last:
        new_solution, new_residual = refs
    else:
        new_solution, new_residual, rounded_ref, unit_q_ref, unit_p_ref, new_known = refs
    site_count = mapped_ref.shape[0]
    half = mapped_ref.shape[1] // 2
    sums = add_pairs(part_refs)

    def row(ref, index):
        return ref[index:index + 1]

    squared = row(sums, 0)
    held_by_new = (row(sums, 1), row(sums, 2))
    coefs = [(row(sums, 3 + 2 * j), row(sums, 4 + 2 * j)) for j in range(count)]
    with_held = [(row(known_ref, 3 * j), row(known_ref, 3 * j + 1)) for j in range(count)]
    short = [row(known_ref, 3 * j + 2) for j in range(count)]
    pairs, place = {}, 3 * count
    for j in range(count):
        for i in range(j):
            pairs[i, j] = (row(known_ref, place), row(known_ref, place + 1))
            place += 2
    for j, coef in enumerate(coefs):
        size = coef[0] * coef[0] + coef[1] * coef[1]
        squared = squared - size * (1.0 + short[j])
        held_by_new = minus(held_by_new, conj_times(coef, with_held[j]))
        for i in range(j):
            squared = squared + 2.0 * conj_times(coefs[i], times(pairs[i, j], coef))[0]
    norm_square = squared + 1e-06
    factor = 1.0 / jnp.sqrt(norm_square)
    alpha = (held_by_new[0] * factor, held_by_new[1] * factor)
    if not last:
        with_new = []
        for j, coef in enumerate(coefs):
            left = (coef[0] * short[j], coef[1] * short[j])
            for i in range(count):
                if i != j:
                    pair = pairs[j, i] if j < i else (pairs[i, j][0], -pairs[i, j][1])
                    left = minus(left, times(pair, coefs[i]))
            with_new.append((left[0] * factor, left[1] * factor))
        new_short = 1e-06 / norm_square
        rows = []
        for j in range(count):
            rows += minus(with_held[j], times(with_new[j], alpha))
            rows.append(short[j])
        rows += [alpha[0] * new_short, alpha[1] * new_short, new_short]
        for j in range(count):
            for i in range(j):
                rows += pairs[i, j]
        for pair in with_new:
            rows += pair
        for index, value in enumerate(rows):
            new_known[index:index + 1] = value
    for site in range(site_count):
        mapped = mapped_ref[site]
        held = residual_ref[site]
        direction = held
        for number, (coef_re, coef_im) in enumerate(coefs):
            mapped = mapped - scaled(basis_q[number][site], coef_re, coef_im, half)
            direction = direction - scaled(basis_p[number][site], coef_re, coef_im, half)
        unit_q = mapped * factor
        unit_p = direction * factor
        change = scaled(unit_p, *alpha, half)
        new_solution[site] = change if solution_ref is None else solution_ref[site] + change
        held = held - scaled(unit_q, *alpha, half)
        new_residual[site] = held
        if not last:
            rounded_ref[site] = held.astype(jnp.bfloat16)
            unit_q_ref[site] = unit_q
            unit_p_ref[site] = unit_p


def add_pairs(refs):
    values = [ref[...] for ref in refs]
    while len(values) > 1:
        values = [values[i] + values[i + 1] for i in range(0, len(values), 2)]
    return values[0]


def add_kernel(*refs):
    refs[-1][...] = add_pairs(refs[:-1])


def gather_sums(sums, device_count):
    step = 1
    while step < device_count:
        step *= 4
    if step != device_count or device_count > 16:
        return [lax.psum(sums, "ta")]
    while step > 1:
        step //= 4
        parts = [sums]
        for turn in (1, 2, 3):
            pairs = [(device, device ^ (turn * step)) for device in range(device_count)]
            parts.append(send(sums, pairs))
        if step > 1:
            shape = jax.ShapeDtypeStruct(sums.shape, jnp.float32)
            sums = whole_call(add_kernel, shape, parts, [VMEM] * 4)
    return parts


def shards(fine_source, projectors, stencil_links, quark_mass):
    _, site_count, comp_count, _ = stencil_links.shape
    plane_count, local_columns = fine_source.shape[:2]
    rhs_count = fine_source.shape[5]
    block_count = projectors.shape[1] // site_count
    chip_count = plane_count // 2
    paired = local_columns * 2 == block_count and local_columns % 8 == 0
    if paired and chip_count & (chip_count - 1) == 0:
        source, rounded = paired_restriction(fine_source, projectors, comp_count)
    else:
        source = general_restriction(
            fine_source, projectors, comp_count, site_count, block_count
        )
        rounded = source.astype(jnp.bfloat16)
    links = stencil_links[0]
    ring = [
        (plane, plane // LZ * LZ + (plane + 1) % LZ) for plane in range(plane_count)
    ]
    back = [(target, origin) for origin, target in ring]
    later = [(plane, (plane + LZ) % plane_count) for plane in range(plane_count)]
    earlier = [(target, origin) for origin, target in later]

    def shape(*sizes, dtype=jnp.float32):
        return jax.ShapeDtypeStruct(sizes, dtype)

    width = 2 * comp_count
    full = shape(site_count, width, rhs_count)
    low = shape(site_count, width, rhs_count, dtype=jnp.bfloat16)
    residual = source
    total = None
    basis_q, basis_p = [], []
    for iteration in range(ITERS):
        last = iteration == ITERS - 1
        nearby = [send(rounded, back), send(rounded, ring)]
        nearby.append(send(rounded, earlier))
        if plane_count > 2 * LZ:
            nearby.append(send(rounded, later))
        packed = (site_count, width, 2 * rhs_count)
        partial = whole_call(
            slice_kernel,
            full,
            (quark_mass, links, rounded),
            [SMEM, VMEM, VMEM],
            [pltpu.VMEM((1,) + packed, jnp.bfloat16)],
        )
        operands = [links, partial, residual, *nearby, *basis_q]
        mapped, sums = whole_call(
            lambda *refs: remote_kernel(iteration, len(nearby), *refs),
            (full, shape(-(-(3 + 2 * iteration) // 8) * 8, rhs_count)),
            operands,
            [VMEM] * len(operands),
            [pltpu.VMEM((len(nearby),) + packed, jnp.bfloat16)],
        )
        parts = gather_sums(sums, plane_count)
        operands = [*parts, mapped, residual, *basis_q, *basis_p]
        if iteration:
            operands += [total, known]
        known_rows = -(-(3 * (iteration + 1) + iteration * (iteration + 1)) // 8) * 8
        results = (full, full)
        if not last:
            results += (low, full, full, shape(known_rows, rhs_count))
        outs = whole_call(
            lambda *refs: update_kernel(iteration, last, len(parts), *refs),
            results,
            operands,
            [VMEM] * len(operands),
        )
        total, residual = outs[:2]
        if not last:
            rounded, known = outs[2], outs[5]
            basis_q.append(outs[3])
            basis_p.append(outs[4])
    return total[None], residual[None]


def solution(mesh):
    return jax.shard_map(
        shards,
        mesh=mesh,
        in_specs=(
            P("cfg", "ta", None, None, None, None),
            P(("cfg", "ta"), None, None),
            P(("cfg", "ta"), None, None, None),
            P("cfg"),
        ),
        out_specs=(P(("cfg", "ta"), None, None, None), P(("cfg", "ta"), None, None, None)),
        check_vma=False,
    )
```

```python
import math

import jax
import jax.numpy as jnp
from jax import lax
from jax.experimental import pallas as pl
from jax.experimental.pallas import tpu as pltpu
from jax.sharding import PartitionSpec as P


LX = 4
LZ = 8
ITERS = 3
LANES = 128
PROJ_STEPS = (6, 3, 7, 1, 5, 2, 4)
SOURCE_STEPS = (6, 3, 7, 5, 4, 1, 2)

VMEM = pl.BlockSpec(memory_space=pltpu.VMEM)
SMEM = pl.BlockSpec(memory_space=pltpu.SMEM)


def send(value, pairs):
    return lax.ppermute(value, "ta", pairs)


def whole_call(body, out_shape, operands, specs, scratch=()):
    return pl.pallas_call(
        body,
        out_shape=out_shape,
        in_specs=specs,
        out_specs=jax.tree.map(lambda _: VMEM, out_shape),
        scratch_shapes=list(scratch),
        compiler_params=pltpu.CompilerParams(vmem_limit_bytes=6 * 1024 * 1024),
    )(*operands)


def unpack_rows(values, rows_ref, pair_count, fine_count):
    column_count = values.shape[0]
    lane = lax.broadcasted_iota(jnp.int32, (column_count, LANES), 1)
    tiles = [values[:, t * LANES:(t + 1) * LANES] for t in range(values.shape[1] // LANES)]

    def window(start, target):
        tile, offset = divmod(start, LANES)
        shift = (target - offset) % LANES
        piece = pltpu.roll(tiles[tile], shift, 1) if shift else tiles[tile]
        if offset + fine_count > LANES:
            after = pltpu.roll(tiles[tile + 1], shift, 1) if shift else tiles[tile + 1]
            piece = jnp.where(lane < target + LANES - offset, piece, after)
        return piece

    for pair in range(pair_count):
        base = (pair * 2 // pair_count) * fine_count
        start = pair * 2 * fine_count
        first = window(start, base)
        second = window(start + fine_count, base + 2 * fine_count)
        row = jnp.where((lane >= base) & (lane < base + fine_count), first, 0.0)
        inside = (lane >= base + 2 * fine_count) & (lane < base + 3 * fine_count)
        row = jnp.where(inside, second, row)
        rows_ref[pl.ds(pair, column_count, stride=pair_count), :] = row


def step_order(chip_count, wanted):
    steps = list(range(1, chip_count))
    return list(wanted) if sorted(wanted) == steps else steps


def split_kernel(device_ref, proj_ref, *out_refs):
    chip = device_ref[0] // 2
    for step, out_ref in enumerate(out_refs):
        out_ref[...] = proj_ref[chip ^ step]


def restrict_kernel(step, device_ref, proj_ref, fine_ref, other_ref, source_ref, rows_ref):
    column_count = proj_ref.shape[0]
    local_count, comp_rows, rhs_count = fine_ref.shape[1:]
    half = comp_rows // 2
    fine_count = half // 2
    pair_count = proj_ref.shape[1] // (2 * fine_count)
    chip = (device_ref[0] // 2) ^ step
    parity = device_ref[0] % 2
    values = proj_ref[...].astype(jnp.float32)
    for core in range(column_count // local_count):
        unpack_rows(
            values[core * local_count:(core + 1) * local_count],
            rows_ref.at[core],
            pair_count,
            fine_count,
        )
    total = jnp.zeros((pair_count, 2 * rhs_count), jnp.float32)
    for core, ref, index in ((parity, fine_ref, 2 * chip + parity), (1 - parity, other_ref, chip)):
        for column in range(local_count):
            weights = rows_ref[core, pl.ds(column * pair_count, pair_count), :]
            weights = weights[:, :comp_rows].astype(jnp.bfloat16)
            block = ref[index, column]
            real, imag = block[:half], block[half:]
            right = jnp.concatenate(
                [
                    jnp.concatenate([real, imag], axis=1),
                    jnp.concatenate([imag, -real], axis=1),
                ],
                axis=0,
            )
            total = total + jnp.dot(weights, right, preferred_element_type=jnp.float32)
    source_ref[:pair_count] = total[:, :rhs_count]
    source_ref[pair_count:] = total[:, rhs_count:]


def round_kernel(*refs):
    for number, part in enumerate(refs[:-1]):
        refs[-1][number] = part[...].astype(jnp.bfloat16)


def join_kernel(steps, device_ref, *refs):
    parts, (source_ref, rounded_ref, late_ref) = refs[:-3], refs[-3:]
    round_kernel(*parts[len(parts) - late_ref.shape[0]:], late_ref)
    chip = device_ref[0] // 2
    for step, part in zip(steps, parts):
        source_ref[chip ^ step] = part[...]
        rounded_ref[chip ^ step] = part[...].astype(jnp.bfloat16)


def paired_restriction(fine_source, projectors, comp_count):
    plane_count, local_columns = fine_source.shape[:2]
    rhs_count = fine_source.shape[-1]
    width = projectors.shape[2]
    chip_count = plane_count // 2
    device = lax.axis_index("ta").astype(jnp.int32)
    place = device.reshape(1)
    low = jnp.bfloat16

    def swap(value, bits):
        return send(value, [(other, other ^ bits) for other in range(plane_count)])

    given = whole_call(
        split_kernel,
        [jax.ShapeDtypeStruct((2 * local_columns, width), low)] * chip_count,
        (place, projectors.reshape(chip_count, 2 * local_columns, width)),
        [SMEM, VMEM],
    )
    order = step_order(chip_count, PROJ_STEPS)
    moved = {0: given[0]}
    for step in order:
        moved[step] = swap(given[step], 2 * step)
    fine = fine_source.reshape(plane_count, local_columns, 2 * comp_count, rhs_count)
    halves = fine.reshape((chip_count, 2) + fine.shape[1:])
    other = swap(lax.dynamic_index_in_dim(halves, 1 - device % 2, axis=1, keepdims=False), 1)
    steps = step_order(chip_count, SOURCE_STEPS) + [0]
    parts = {}
    for step in steps:
        part = whole_call(
            lambda *refs: restrict_kernel(step, *refs),
            jax.ShapeDtypeStruct((2 * comp_count, rhs_count), jnp.float32),
            (place, moved[step], fine, other),
            [SMEM, VMEM, VMEM, VMEM],
            [pltpu.VMEM((2, local_columns * comp_count, LANES), jnp.float32)],
        )
        parts[step] = swap(part, 2 * step) if step else part
    shape = (chip_count, 2 * comp_count, rhs_count)
    half = jax.ShapeDtypeStruct((chip_count // 2,) + shape[1:], low)
    pieces = [steps[:chip_count // 2], steps[chip_count // 2:]]
    first = whole_call(
        round_kernel, half, [parts[step] for step in pieces[0]], [VMEM] * (chip_count // 2)
    )
    source, rounded, second = whole_call(
        lambda *refs: join_kernel(steps, *refs),
        (jax.ShapeDtypeStruct(shape, jnp.float32), jax.ShapeDtypeStruct(shape, low), half),
        (place, *(parts[step] for step in steps)),
        [SMEM] + [VMEM] * chip_count,
    )
    return source, rounded, pieces, (first, second)


def real_weights(proj_view):
    proj_re = proj_view[..., 0, :]
    proj_im = proj_view[..., 1, :]
    first_row = jnp.stack([proj_re, proj_im], axis=-4)
    second_row = jnp.stack([-proj_im, proj_re], axis=-4)
    return jnp.stack([first_row, second_row], axis=-5)


def general_restriction(fine_source, projectors, comp_count, site_count, block_count):
    null_count = comp_count // 2
    plane_count, local_columns = fine_source.shape[:2]
    fine_count, rhs_count = fine_source.shape[4:]
    moved_proj = lax.all_to_all(projectors, "ta", split_axis=1, concat_axis=0, tiled=True)
    group_size = math.gcd(block_count, local_columns)
    groups = local_columns // group_size
    weights = real_weights(
        moved_proj.reshape(plane_count, groups, group_size, 2, null_count, 2, fine_count)
    )
    fine_local = fine_source.reshape(plane_count, groups, group_size, 2, 2, fine_count, rhs_count)
    partial_sums = jnp.einsum(
        "pmgdchvk,pmgchkr->pmdhvr", weights, fine_local, preferred_element_type=jnp.float32
    )
    partial_sums = partial_sums.reshape(plane_count, groups, 2 * comp_count, rhs_count)
    collected = lax.all_to_all(partial_sums, "ta", split_axis=0, concat_axis=1, tiled=True)
    return jnp.sum(
        collected.reshape(site_count, block_count // group_size, 2 * comp_count, rhs_count), axis=1
    )


def fold(value):
    return jnp.sum(value.reshape(-1, 8, value.shape[-1]), axis=0)


def cross(left, right, half):
    left_re, left_im = left[:half], left[half:]
    right_re, right_im = right[:half], right[half:]
    return (
        fold(left_re * right_re + left_im * right_im),
        fold(left_re * right_im - left_im * right_re),
    )


def pack_vector(vector, packed_ref, number, sites=None):
    half = vector.shape[1] // 2
    rhs_count = vector.shape[2]
    for index, site in enumerate(sites or range(vector.shape[0])):
        real = vector[index, :half]
        imag = vector[index, half:]
        packed_ref[number, site, :half, :rhs_count] = real
        packed_ref[number, site, :half, rhs_count:] = imag
        packed_ref[number, site, half:, :rhs_count] = -imag
        packed_ref[number, site, half:, rhs_count:] = real


def stacked(product):
    rhs_count = product.shape[1] // 2
    return jnp.concatenate([product[:, :rhs_count], product[:, rhs_count:]], axis=0)


def slice_kernel(mass_ref, links_ref, own_ref, mapped_ref, packed_ref):
    site_count, _, _ = links_ref.shape
    line_count = site_count // LX
    mass = mass_ref[0]
    pack_vector(own_ref, packed_ref, 0)
    for site in range(site_count):
        line, column = divmod(site, LX)
        places = [
            (line, column),
            (line, (column + 1) % LX),
            (line, (column - 1) % LX),
            ((line + 1) % line_count, column),
            ((line - 1) % line_count, column),
        ]
        right = jnp.concatenate([packed_ref[0, y * LX + x] for y, x in places], axis=0)
        product = jnp.dot(
            links_ref[site, :, :right.shape[0]], right, preferred_element_type=jnp.float32
        )
        mapped_ref[site] = stacked(product) + mass * own_ref[site].astype(jnp.float32)


def remote_kernel(count, near, pieces, device_ref, links_ref, partial_ref, residual_ref, *refs):
    mapped_ref, sums_ref, packed_ref = refs[-3:]
    vectors = len(refs) - 3 - count
    basis = refs[vectors:vectors + count]
    site_count, comp_count, width = links_ref.shape
    rhs_count = residual_ref.shape[2]
    parity = device_ref[0] % 2
    for number in range(2):
        pack_vector(refs[number], packed_ref, (parity, 1 - parity)[number])
    if pieces:
        partner = (device_ref[0] + LZ) % (2 * LZ) // 2
        for number, steps in enumerate(pieces):
            pack_vector(refs[2 + number], packed_ref, 2, [partner ^ step for step in steps])
    else:
        for number in range(2, near):
            pack_vector(refs[number], packed_ref, number)
    start = width - 8 * comp_count
    spare = start % LANES
    totals = [jnp.zeros((8, rhs_count), jnp.float32) for _ in range(3 + 2 * count)]
    for site in range(site_count):
        blocks = [packed_ref[n, site] for n in (0, 1, 2, near - 1)]
        if spare:
            blocks.insert(0, jnp.zeros((spare, 2 * rhs_count), jnp.bfloat16))
        right = jnp.concatenate(blocks, axis=0)
        product = jnp.dot(
            links_ref[site, :, start - spare:], right, preferred_element_type=jnp.float32
        )
        mapped = partial_ref[site] + stacked(product)
        mapped_ref[site] = mapped
        held = residual_ref[site]
        parts = [fold(mapped * mapped), *cross(mapped, held, comp_count)]
        for earlier in basis:
            parts += cross(earlier[site], mapped, comp_count)
        totals = [total + part for total, part in zip(totals, parts)]
    sums_ref[...] = jnp.concatenate(
        [jnp.sum(total, axis=0, keepdims=True) for total in totals]
        + [jnp.zeros((sums_ref.shape[0] - len(totals), rhs_count), jnp.float32)],
        axis=0,
    )


def scaled(vector, factor_re, factor_im, half):
    vector_re, vector_im = vector[:half], vector[half:]
    return jnp.concatenate(
        [
            factor_re * vector_re - factor_im * vector_im,
            factor_re * vector_im + factor_im * vector_re,
        ],
        axis=0,
    )


def times(left, right):
    return left[0] * right[0] - left[1] * right[1], left[0] * right[1] + left[1] * right[0]


def conj_times(left, right):
    return left[0] * right[0] + left[1] * right[1], left[0] * right[1] - left[1] * right[0]


def minus(left, right):
    return left[0] - right[0], left[1] - right[1]


def update_kernel(count, last, parts, *refs):
    refs = list(refs)
    part_refs = [refs.pop(0) for _ in range(parts)]
    mapped_ref, residual_ref = refs.pop(0), refs.pop(0)
    basis_q = [refs.pop(0) for _ in range(count)]
    basis_p = [refs.pop(0) for _ in range(count)]
    solution_ref, known_ref = (refs.pop(0), refs.pop(0)) if count else (None, None)
    if last:
        new_solution, new_residual = refs
    else:
        new_solution, new_residual, rounded_ref, unit_q_ref, unit_p_ref, new_known = refs
    site_count = mapped_ref.shape[0]
    half = mapped_ref.shape[1] // 2
    sums = add_pairs(part_refs)

    def row(ref, index):
        return ref[index:index + 1]

    squared = row(sums, 0)
    held_by_new = (row(sums, 1), row(sums, 2))
    coefs = [(row(sums, 3 + 2 * j), row(sums, 4 + 2 * j)) for j in range(count)]
    with_held = [(row(known_ref, 3 * j), row(known_ref, 3 * j + 1)) for j in range(count)]
    short = [row(known_ref, 3 * j + 2) for j in range(count)]
    pairs, place = {}, 3 * count
    for j in range(count):
        for i in range(j):
            pairs[i, j] = (row(known_ref, place), row(known_ref, place + 1))
            place += 2
    for j, coef in enumerate(coefs):
        size = coef[0] * coef[0] + coef[1] * coef[1]
        squared = squared - size * (1.0 + short[j])
        held_by_new = minus(held_by_new, conj_times(coef, with_held[j]))
        for i in range(j):
            squared = squared + 2.0 * conj_times(coefs[i], times(pairs[i, j], coef))[0]
    norm_square = squared + 1e-06
    factor = 1.0 / jnp.sqrt(norm_square)
    alpha = (held_by_new[0] * factor, held_by_new[1] * factor)
    if not last:
        with_new = []
        for j, coef in enumerate(coefs):
            left = (coef[0] * short[j], coef[1] * short[j])
            for i in range(count):
                if i != j:
                    pair = pairs[j, i] if j < i else (pairs[i, j][0], -pairs[i, j][1])
                    left = minus(left, times(pair, coefs[i]))
            with_new.append((left[0] * factor, left[1] * factor))
        new_short = 1e-06 / norm_square
        rows = []
        for j in range(count):
            rows += minus(with_held[j], times(with_new[j], alpha))
            rows.append(short[j])
        rows += [alpha[0] * new_short, alpha[1] * new_short, new_short]
        for j in range(count):
            for i in range(j):
                rows += pairs[i, j]
        for pair in with_new:
            rows += pair
        for index, value in enumerate(rows):
            new_known[index:index + 1] = value
    for site in range(site_count):
        mapped = mapped_ref[site]
        held = residual_ref[site]
        direction = held
        for number, (coef_re, coef_im) in enumerate(coefs):
            mapped = mapped - scaled(basis_q[number][site], coef_re, coef_im, half)
            direction = direction - scaled(basis_p[number][site], coef_re, coef_im, half)
        unit_q = mapped * factor
        unit_p = direction * factor
        change = scaled(unit_p, *alpha, half)
        new_solution[site] = change if solution_ref is None else solution_ref[site] + change
        held = held - scaled(unit_q, *alpha, half)
        new_residual[site] = held
        if not last:
            rounded_ref[site] = held.astype(jnp.bfloat16)
            unit_q_ref[site] = unit_q
            unit_p_ref[site] = unit_p


def add_pairs(refs):
    values = [ref[...] for ref in refs]
    while len(values) > 1:
        values = [values[i] + values[i + 1] for i in range(0, len(values), 2)]
    return values[0]


def add_kernel(*refs):
    refs[-1][...] = add_pairs(refs[:-1])


def gather_sums(sums, device_count):
    step = 1
    while step < device_count:
        step *= 4
    if step != device_count or device_count > 16:
        return [lax.psum(sums, "ta")]
    while step > 1:
        step //= 4
        parts = [sums]
        for turn in (1, 2, 3):
            pairs = [(device, device ^ (turn * step)) for device in range(device_count)]
            parts.append(send(sums, pairs))
        if step > 1:
            shape = jax.ShapeDtypeStruct(sums.shape, jnp.float32)
            sums = whole_call(add_kernel, shape, parts, [VMEM] * 4)
    return parts


def shards(fine_source, projectors, stencil_links, quark_mass):
    _, site_count, comp_count, _ = stencil_links.shape
    plane_count, local_columns = fine_source.shape[:2]
    rhs_count = fine_source.shape[5]
    block_count = projectors.shape[1] // site_count
    chip_count = plane_count // 2
    paired = local_columns * 2 == block_count and local_columns % 8 == 0
    if paired and chip_count & (chip_count - 1) == 0:
        source, rounded, pieces, halves = paired_restriction(fine_source, projectors, comp_count)
    else:
        source = general_restriction(
            fine_source, projectors, comp_count, site_count, block_count
        )
        rounded = source.astype(jnp.bfloat16)
        pieces = None
    if plane_count != 2 * LZ:
        pieces = None
    links = stencil_links[0]
    inner = [(plane, plane ^ 1) for plane in range(plane_count)]
    outer = []
    for plane in range(plane_count):
        turn = 1 if plane % 2 else -1
        outer.append((plane, plane // LZ * LZ + (plane + turn) % LZ))
    later = [(plane, (plane + LZ) % plane_count) for plane in range(plane_count)]
    earlier = [(target, origin) for origin, target in later]

    def shape(*sizes, dtype=jnp.float32):
        return jax.ShapeDtypeStruct(sizes, dtype)

    width = 2 * comp_count
    full = shape(site_count, width, rhs_count)
    low = shape(site_count, width, rhs_count, dtype=jnp.bfloat16)
    device = lax.axis_index("ta").astype(jnp.int32).reshape(1)
    residual = source
    total = None
    basis_q, basis_p = [], []
    for iteration in range(ITERS):
        last = iteration == ITERS - 1
        nearby = [send(rounded, inner), send(rounded, outer)]
        parted = pieces if iteration == 0 else None
        near = 3
        if parted:
            nearby.append(send(halves[0], earlier))
            nearby.append(send(halves[1], earlier))
        else:
            nearby.append(send(rounded, earlier))
        if plane_count > 2 * LZ:
            near = 4
            nearby.append(send(rounded, later))
        packed = (site_count, width, 2 * rhs_count)
        partial = whole_call(
            slice_kernel,
            full,
            (quark_mass, links, rounded),
            [SMEM, VMEM, VMEM],
            [pltpu.VMEM((1,) + packed, jnp.bfloat16)],
        )
        operands = [device, links, partial, residual, *nearby, *basis_q]
        mapped, sums = whole_call(
            lambda *refs: remote_kernel(iteration, near, parted, *refs),
            (full, shape(-(-(3 + 2 * iteration) // 8) * 8, rhs_count)),
            operands,
            [SMEM] + [VMEM] * (len(operands) - 1),
            [pltpu.VMEM((near,) + packed, jnp.bfloat16)],
        )
        parts = gather_sums(sums, plane_count)
        operands = [*parts, mapped, residual, *basis_q, *basis_p]
        if iteration:
            operands += [total, known]
        known_rows = -(-(3 * (iteration + 1) + iteration * (iteration + 1)) // 8) * 8
        results = (full, full)
        if not last:
            results += (low, full, full, shape(known_rows, rhs_count))
        outs = whole_call(
            lambda *refs: update_kernel(iteration, last, len(parts), *refs),
            results,
            operands,
            [VMEM] * len(operands),
        )
        total, residual = outs[:2]
        if not last:
            rounded, known = outs[2], outs[5]
            basis_q.append(outs[3])
            basis_p.append(outs[4])
    return total[None], residual[None]


def solution(mesh):
    return jax.shard_map(
        shards,
        mesh=mesh,
        in_specs=(
            P("cfg", "ta", None, None, None, None),
            P(("cfg", "ta"), None, None),
            P(("cfg", "ta"), None, None, None),
            P("cfg"),
        ),
        out_specs=(P(("cfg", "ta"), None, None, None), P(("cfg", "ta"), None, None, None)),
        check_vma=False,
    )
```

```python
import math

import jax
import jax.numpy as jnp
from jax import lax
from jax.experimental import pallas as pl
from jax.experimental.pallas import tpu as pltpu
from jax.sharding import PartitionSpec as P


LX = 4
LZ = 8
ITERS = 3
LANES = 128
PROJ_STEPS = (6, 3, 7, 1, 5, 2, 4)
SOURCE_STEPS = (6, 3, 7, 5, 4, 1, 2)

VMEM = pl.BlockSpec(memory_space=pltpu.VMEM)
SMEM = pl.BlockSpec(memory_space=pltpu.SMEM)


def send(value, pairs):
    return lax.ppermute(value, "ta", pairs)


def whole_call(body, out_shape, operands, specs, scratch=(), out=VMEM):
    return pl.pallas_call(
        body,
        out_shape=out_shape,
        in_specs=specs,
        out_specs=jax.tree.map(lambda _: out, out_shape),
        scratch_shapes=list(scratch),
        compiler_params=pltpu.CompilerParams(vmem_limit_bytes=6 * 1024 * 1024),
    )(*operands)


def unpack_rows(values, rows_ref, pair_count, fine_count):
    column_count = values.shape[0]
    lane = lax.broadcasted_iota(jnp.int32, (column_count, LANES), 1)
    tiles = [values[:, t * LANES:(t + 1) * LANES] for t in range(values.shape[1] // LANES)]

    def window(start, target):
        tile, offset = divmod(start, LANES)
        shift = (target - offset) % LANES
        piece = pltpu.roll(tiles[tile], shift, 1) if shift else tiles[tile]
        if offset + fine_count > LANES:
            after = pltpu.roll(tiles[tile + 1], shift, 1) if shift else tiles[tile + 1]
            piece = jnp.where(lane < target + LANES - offset, piece, after)
        return piece

    for pair in range(pair_count):
        base = (pair * 2 // pair_count) * fine_count
        start = pair * 2 * fine_count
        first = window(start, base)
        second = window(start + fine_count, base + 2 * fine_count)
        row = jnp.where((lane >= base) & (lane < base + fine_count), first, 0.0)
        inside = (lane >= base + 2 * fine_count) & (lane < base + 3 * fine_count)
        row = jnp.where(inside, second, row)
        rows_ref[pl.ds(pair, column_count, stride=pair_count), :] = row


def step_order(chip_count, wanted):
    steps = list(range(1, chip_count))
    return list(wanted) if sorted(wanted) == steps else steps


def split_kernel(device_ref, proj_ref, *out_refs):
    chip = device_ref[0] // 2
    for step, out_ref in enumerate(out_refs):
        out_ref[...] = proj_ref[chip ^ step]


def restrict_kernel(step, device_ref, proj_ref, fine_ref, other_ref, source_ref, rows_ref):
    column_count = proj_ref.shape[0]
    local_count, comp_rows, rhs_count = fine_ref.shape[1:]
    half = comp_rows // 2
    fine_count = half // 2
    pair_count = proj_ref.shape[1] // (2 * fine_count)
    chip = (device_ref[0] // 2) ^ step
    parity = device_ref[0] % 2
    values = proj_ref[...].astype(jnp.float32)
    for core in range(column_count // local_count):
        unpack_rows(
            values[core * local_count:(core + 1) * local_count],
            rows_ref.at[core],
            pair_count,
            fine_count,
        )
    total = jnp.zeros((pair_count, 2 * rhs_count), jnp.float32)
    for core, ref, index in ((parity, fine_ref, 2 * chip + parity), (1 - parity, other_ref, chip)):
        for column in range(local_count):
            weights = rows_ref[core, pl.ds(column * pair_count, pair_count), :]
            weights = weights[:, :comp_rows].astype(jnp.bfloat16)
            block = ref[index, column]
            real, imag = block[:half], block[half:]
            right = jnp.concatenate(
                [
                    jnp.concatenate([real, imag], axis=1),
                    jnp.concatenate([imag, -real], axis=1),
                ],
                axis=0,
            )
            total = total + jnp.dot(weights, right, preferred_element_type=jnp.float32)
    source_ref[:pair_count] = total[:, :rhs_count]
    source_ref[pair_count:] = total[:, rhs_count:]


def round_kernel(*refs):
    for number, part in enumerate(refs[:-1]):
        refs[-1][number] = part[...].astype(jnp.bfloat16)


def join_kernel(steps, device_ref, *refs):
    parts, (source_ref, rounded_ref, late_ref) = refs[:-3], refs[-3:]
    round_kernel(*parts[len(parts) - late_ref.shape[0]:], late_ref)
    chip = device_ref[0] // 2
    for step, part in zip(steps, parts):
        source_ref[chip ^ step] = part[...]
        rounded_ref[chip ^ step] = part[...].astype(jnp.bfloat16)


def paired_restriction(fine_source, projectors, comp_count):
    plane_count, local_columns = fine_source.shape[:2]
    rhs_count = fine_source.shape[-1]
    width = projectors.shape[2]
    chip_count = plane_count // 2
    device = lax.axis_index("ta").astype(jnp.int32)
    place = device.reshape(1)
    low = jnp.bfloat16

    def swap(value, bits):
        return send(value, [(other, other ^ bits) for other in range(plane_count)])

    given = whole_call(
        split_kernel,
        [jax.ShapeDtypeStruct((2 * local_columns, width), low)] * chip_count,
        (place, projectors.reshape(chip_count, 2 * local_columns, width)),
        [SMEM, VMEM],
    )
    order = step_order(chip_count, PROJ_STEPS)
    moved = {0: given[0]}
    for step in order:
        moved[step] = swap(given[step], 2 * step)
    fine = fine_source.reshape(plane_count, local_columns, 2 * comp_count, rhs_count)
    halves = fine.reshape((chip_count, 2) + fine.shape[1:])
    other = swap(lax.dynamic_index_in_dim(halves, 1 - device % 2, axis=1, keepdims=False), 1)
    steps = step_order(chip_count, SOURCE_STEPS) + [0]
    parts = {}
    for step in steps:
        part = whole_call(
            lambda *refs: restrict_kernel(step, *refs),
            jax.ShapeDtypeStruct((2 * comp_count, rhs_count), jnp.float32),
            (place, moved[step], fine, other),
            [SMEM, VMEM, VMEM, VMEM],
            [pltpu.VMEM((2, local_columns * comp_count, LANES), jnp.float32)],
        )
        parts[step] = swap(part, 2 * step) if step else part
    shape = (chip_count, 2 * comp_count, rhs_count)
    half = jax.ShapeDtypeStruct((chip_count // 2,) + shape[1:], low)
    pieces = [steps[:chip_count // 2], steps[chip_count // 2:]]
    first = whole_call(
        round_kernel, half, [parts[step] for step in pieces[0]], [VMEM] * (chip_count // 2)
    )
    source, rounded, second = whole_call(
        lambda *refs: join_kernel(steps, *refs),
        (jax.ShapeDtypeStruct(shape, jnp.float32), jax.ShapeDtypeStruct(shape, low), half),
        (place, *(parts[step] for step in steps)),
        [SMEM] + [VMEM] * chip_count,
    )
    return source, rounded, pieces, (first, second)


def real_weights(proj_view):
    proj_re = proj_view[..., 0, :]
    proj_im = proj_view[..., 1, :]
    first_row = jnp.stack([proj_re, proj_im], axis=-4)
    second_row = jnp.stack([-proj_im, proj_re], axis=-4)
    return jnp.stack([first_row, second_row], axis=-5)


def general_restriction(fine_source, projectors, comp_count, site_count, block_count):
    null_count = comp_count // 2
    plane_count, local_columns = fine_source.shape[:2]
    fine_count, rhs_count = fine_source.shape[4:]
    moved_proj = lax.all_to_all(projectors, "ta", split_axis=1, concat_axis=0, tiled=True)
    group_size = math.gcd(block_count, local_columns)
    groups = local_columns // group_size
    weights = real_weights(
        moved_proj.reshape(plane_count, groups, group_size, 2, null_count, 2, fine_count)
    )
    fine_local = fine_source.reshape(plane_count, groups, group_size, 2, 2, fine_count, rhs_count)
    partial_sums = jnp.einsum(
        "pmgdchvk,pmgchkr->pmdhvr", weights, fine_local, preferred_element_type=jnp.float32
    )
    partial_sums = partial_sums.reshape(plane_count, groups, 2 * comp_count, rhs_count)
    collected = lax.all_to_all(partial_sums, "ta", split_axis=0, concat_axis=1, tiled=True)
    return jnp.sum(
        collected.reshape(site_count, block_count // group_size, 2 * comp_count, rhs_count), axis=1
    )


def fold(value):
    return jnp.sum(value.reshape(-1, 8, value.shape[-1]), axis=0)


def cross(left, right, half):
    left_re, left_im = left[:half], left[half:]
    right_re, right_im = right[:half], right[half:]
    return (
        fold(left_re * right_re + left_im * right_im),
        fold(left_re * right_im - left_im * right_re),
    )


def pack_vector(vector, packed_ref, number, sites=None):
    half = vector.shape[1] // 2
    rhs_count = vector.shape[2]
    for index, site in enumerate(sites or range(vector.shape[0])):
        real = vector[index, :half]
        imag = vector[index, half:]
        packed_ref[number, site, :half, :rhs_count] = real
        packed_ref[number, site, :half, rhs_count:] = imag
        packed_ref[number, site, half:, :rhs_count] = -imag
        packed_ref[number, site, half:, rhs_count:] = real


def stacked(product):
    rhs_count = product.shape[1] // 2
    return jnp.concatenate([product[:, :rhs_count], product[:, rhs_count:]], axis=0)


def slice_kernel(mass_ref, links_ref, own_ref, mapped_ref, packed_ref):
    site_count, _, _ = links_ref.shape
    line_count = site_count // LX
    mass = mass_ref[0]
    pack_vector(own_ref, packed_ref, 0)
    for site in range(site_count):
        line, column = divmod(site, LX)
        places = [
            (line, column),
            (line, (column + 1) % LX),
            (line, (column - 1) % LX),
            ((line + 1) % line_count, column),
            ((line - 1) % line_count, column),
        ]
        right = jnp.concatenate([packed_ref[0, y * LX + x] for y, x in places], axis=0)
        product = jnp.dot(
            links_ref[site, :, :right.shape[0]], right, preferred_element_type=jnp.float32
        )
        mapped_ref[site] = stacked(product) + mass * own_ref[site].astype(jnp.float32)


def remote_kernel(count, near, pieces, device_ref, links_ref, partial_ref, residual_ref, *refs):
    mapped_ref, sums_ref, packed_ref = refs[-3:]
    vectors = len(refs) - 3 - count
    basis = refs[vectors:vectors + count]
    site_count, comp_count, width = links_ref.shape
    rhs_count = residual_ref.shape[2]
    parity = device_ref[0] % 2
    for number in range(2):
        pack_vector(refs[number], packed_ref, (parity, 1 - parity)[number])
    if pieces:
        partner = (device_ref[0] + LZ) % (2 * LZ) // 2
        for number, steps in enumerate(pieces):
            pack_vector(refs[2 + number], packed_ref, 2, [partner ^ step for step in steps])
    else:
        for number in range(2, near):
            pack_vector(refs[number], packed_ref, number)
    start = width - 8 * comp_count
    spare = start % LANES
    totals = [jnp.zeros((8, rhs_count), jnp.float32) for _ in range(3 + 2 * count)]
    for site in range(site_count):
        blocks = [packed_ref[n, site] for n in (0, 1, 2, near - 1)]
        if spare:
            blocks.insert(0, jnp.zeros((spare, 2 * rhs_count), jnp.bfloat16))
        right = jnp.concatenate(blocks, axis=0)
        product = jnp.dot(
            links_ref[site, :, start - spare:], right, preferred_element_type=jnp.float32
        )
        mapped = partial_ref[site] + stacked(product)
        mapped_ref[site] = mapped
        held = residual_ref[site]
        parts = [fold(mapped * mapped), *cross(mapped, held, comp_count)]
        for earlier in basis:
            parts += cross(earlier[site], mapped, comp_count)
        totals = [total + part for total, part in zip(totals, parts)]
    sums_ref[...] = jnp.concatenate(
        [jnp.sum(total, axis=0, keepdims=True) for total in totals]
        + [jnp.zeros((sums_ref.shape[0] - len(totals), rhs_count), jnp.float32)],
        axis=0,
    )


def scaled(vector, factor_re, factor_im, half):
    vector_re, vector_im = vector[:half], vector[half:]
    return jnp.concatenate(
        [
            factor_re * vector_re - factor_im * vector_im,
            factor_re * vector_im + factor_im * vector_re,
        ],
        axis=0,
    )


def times(left, right):
    return left[0] * right[0] - left[1] * right[1], left[0] * right[1] + left[1] * right[0]


def conj_times(left, right):
    return left[0] * right[0] + left[1] * right[1], left[0] * right[1] - left[1] * right[0]


def minus(left, right):
    return left[0] - right[0], left[1] - right[1]


def update_kernel(count, last, parts, *refs):
    refs = list(refs)
    part_refs = [refs.pop(0) for _ in range(parts)]
    mapped_ref, residual_ref = refs.pop(0), refs.pop(0)
    basis_q = [refs.pop(0) for _ in range(count)]
    basis_p = [refs.pop(0) for _ in range(count)]
    solution_ref, known_ref = (refs.pop(0), refs.pop(0)) if count else (None, None)
    copies = []
    if last:
        whole_solution, whole_residual, new_solution, new_residual, semaphores = refs
    else:
        new_solution, new_residual, rounded_ref, unit_q_ref, unit_p_ref, new_known = refs
    site_count = mapped_ref.shape[0]
    half = mapped_ref.shape[1] // 2
    sums = add_pairs(part_refs)

    def row(ref, index):
        return ref[index:index + 1]

    squared = row(sums, 0)
    held_by_new = (row(sums, 1), row(sums, 2))
    coefs = [(row(sums, 3 + 2 * j), row(sums, 4 + 2 * j)) for j in range(count)]
    with_held = [(row(known_ref, 3 * j), row(known_ref, 3 * j + 1)) for j in range(count)]
    short = [row(known_ref, 3 * j + 2) for j in range(count)]
    pairs, place = {}, 3 * count
    for j in range(count):
        for i in range(j):
            pairs[i, j] = (row(known_ref, place), row(known_ref, place + 1))
            place += 2
    for j, coef in enumerate(coefs):
        size = coef[0] * coef[0] + coef[1] * coef[1]
        squared = squared - size * (1.0 + short[j])
        held_by_new = minus(held_by_new, conj_times(coef, with_held[j]))
        for i in range(j):
            squared = squared + 2.0 * conj_times(coefs[i], times(pairs[i, j], coef))[0]
    norm_square = squared + 1e-06
    factor = 1.0 / jnp.sqrt(norm_square)
    alpha = (held_by_new[0] * factor, held_by_new[1] * factor)
    if not last:
        with_new = []
        for j, coef in enumerate(coefs):
            left = (coef[0] * short[j], coef[1] * short[j])
            for i in range(count):
                if i != j:
                    pair = pairs[j, i] if j < i else (pairs[i, j][0], -pairs[i, j][1])
                    left = minus(left, times(pair, coefs[i]))
            with_new.append((left[0] * factor, left[1] * factor))
        new_short = 1e-06 / norm_square
        rows = []
        for j in range(count):
            rows += minus(with_held[j], times(with_new[j], alpha))
            rows.append(short[j])
        rows += [alpha[0] * new_short, alpha[1] * new_short, new_short]
        for j in range(count):
            for i in range(j):
                rows += pairs[i, j]
        for pair in with_new:
            rows += pair
        for index, value in enumerate(rows):
            new_known[index:index + 1] = value
    for site in range(site_count):
        mapped = mapped_ref[site]
        held = residual_ref[site]
        direction = held
        for number, (coef_re, coef_im) in enumerate(coefs):
            mapped = mapped - scaled(basis_q[number][site], coef_re, coef_im, half)
            direction = direction - scaled(basis_p[number][site], coef_re, coef_im, half)
        unit_q = mapped * factor
        unit_p = direction * factor
        change = scaled(unit_p, *alpha, half)
        new_solution[site] = change if solution_ref is None else solution_ref[site] + change
        held = held - scaled(unit_q, *alpha, half)
        new_residual[site] = held
        if last:
            pairs = ((new_solution, whole_solution), (new_residual, whole_residual))
            for number, (local, whole) in enumerate(pairs):
                copies.append(
                    pltpu.make_async_copy(
                        local.at[site], whole.at[site], semaphores.at[number, site]
                    )
                )
                copies[-1].start()
        else:
            rounded_ref[site] = held.astype(jnp.bfloat16)
            unit_q_ref[site] = unit_q
            unit_p_ref[site] = unit_p
    for copy in copies:
        copy.wait()


def add_pairs(refs):
    values = [ref[...] for ref in refs]
    while len(values) > 1:
        values = [values[i] + values[i + 1] for i in range(0, len(values), 2)]
    return values[0]


def add_kernel(*refs):
    refs[-1][...] = add_pairs(refs[:-1])


def gather_sums(sums, device_count):
    step = 1
    while step < device_count:
        step *= 4
    if step != device_count or device_count > 16:
        return [lax.psum(sums, "ta")]
    while step > 1:
        step //= 4
        parts = [sums]
        for turn in (1, 2, 3):
            pairs = [(device, device ^ (turn * step)) for device in range(device_count)]
            parts.append(send(sums, pairs))
        if step > 1:
            shape = jax.ShapeDtypeStruct(sums.shape, jnp.float32)
            sums = whole_call(add_kernel, shape, parts, [VMEM] * 4)
    return parts


def shards(fine_source, projectors, stencil_links, quark_mass):
    _, site_count, comp_count, _ = stencil_links.shape
    plane_count, local_columns = fine_source.shape[:2]
    rhs_count = fine_source.shape[5]
    block_count = projectors.shape[1] // site_count
    chip_count = plane_count // 2
    paired = local_columns * 2 == block_count and local_columns % 8 == 0
    if paired and chip_count & (chip_count - 1) == 0:
        source, rounded, pieces, halves = paired_restriction(fine_source, projectors, comp_count)
    else:
        source = general_restriction(
            fine_source, projectors, comp_count, site_count, block_count
        )
        rounded = source.astype(jnp.bfloat16)
        pieces = None
    if plane_count != 2 * LZ:
        pieces = None
    links = stencil_links[0]
    inner = [(plane, plane ^ 1) for plane in range(plane_count)]
    outer = []
    for plane in range(plane_count):
        turn = 1 if plane % 2 else -1
        outer.append((plane, plane // LZ * LZ + (plane + turn) % LZ))
    later = [(plane, (plane + LZ) % plane_count) for plane in range(plane_count)]
    earlier = [(target, origin) for origin, target in later]

    def shape(*sizes, dtype=jnp.float32):
        return jax.ShapeDtypeStruct(sizes, dtype)

    width = 2 * comp_count
    full = shape(site_count, width, rhs_count)
    low = shape(site_count, width, rhs_count, dtype=jnp.bfloat16)
    device = lax.axis_index("ta").astype(jnp.int32).reshape(1)
    residual = source
    total = None
    basis_q, basis_p = [], []
    for iteration in range(ITERS):
        last = iteration == ITERS - 1
        nearby = [send(rounded, inner), send(rounded, outer)]
        parted = pieces if iteration == 0 else None
        near = 3
        if parted:
            nearby.append(send(halves[0], earlier))
            nearby.append(send(halves[1], earlier))
        else:
            nearby.append(send(rounded, earlier))
        if plane_count > 2 * LZ:
            near = 4
            nearby.append(send(rounded, later))
        packed = (site_count, width, 2 * rhs_count)
        partial = whole_call(
            slice_kernel,
            full,
            (quark_mass, links, rounded),
            [SMEM, VMEM, VMEM],
            [pltpu.VMEM((1,) + packed, jnp.bfloat16)],
        )
        operands = [device, links, partial, residual, *nearby, *basis_q]
        mapped, sums = whole_call(
            lambda *refs: remote_kernel(iteration, near, parted, *refs),
            (full, shape(-(-(3 + 2 * iteration) // 8) * 8, rhs_count)),
            operands,
            [SMEM] + [VMEM] * (len(operands) - 1),
            [pltpu.VMEM((near,) + packed, jnp.bfloat16)],
        )
        parts = gather_sums(sums, plane_count)
        operands = [*parts, mapped, residual, *basis_q, *basis_p]
        if iteration:
            operands += [total, known]
        known_rows = -(-(3 * (iteration + 1) + iteration * (iteration + 1)) // 8) * 8
        results = (full, full)
        if not last:
            results += (low, full, full, shape(known_rows, rhs_count))
        outs = whole_call(
            lambda *refs: update_kernel(iteration, last, len(parts), *refs),
            results,
            operands,
            [VMEM] * len(operands),
            [
                pltpu.VMEM(full.shape, jnp.float32),
                pltpu.VMEM(full.shape, jnp.float32),
                pltpu.SemaphoreType.DMA((2, site_count)),
            ]
            if last
            else [],
            out=pl.BlockSpec(memory_space=pl.ANY) if last else VMEM,
        )
        total, residual = outs[:2]
        if not last:
            rounded, known = outs[2], outs[5]
            basis_q.append(outs[3])
            basis_p.append(outs[4])
    return total[None], residual[None]


def solution(mesh):
    return jax.shard_map(
        shards,
        mesh=mesh,
        in_specs=(
            P("cfg", "ta", None, None, None, None),
            P(("cfg", "ta"), None, None),
            P(("cfg", "ta"), None, None, None),
            P("cfg"),
        ),
        out_specs=(P(("cfg", "ta"), None, None, None), P(("cfg", "ta"), None, None, None)),
        check_vma=False,
    )
```
